32 devices in a mesh: fsdp: 4 (over y, x), tp: 2 (over core), rep: 4 (over z).
Axes of the slice: x: 2, y: 2, z: 4, core: 2. Of those that a mesh axis runs over, the one named last changes fastest.
Arguments:
- tokens: bfloat16 [4096, 5120], P('fsdp', 'rep'), may hold values from -6 to 6
- ref_qkv: bfloat16 [5120, 7168], P(('rep', 'fsdp'), 'tp'), may hold values from -0.078125 to 0.078125
- ref_bias: float32 [7168], P('tp'), may hold values from -9 to 9
- segment_ids: int32 [4, 1024], P('fsdp'), may hold values from 0 to 7, never falling along the last dimension, each value on 1 to 512 neighbouring positions
- policy_key: bfloat16 [5120, 1024], P(('rep', 'fsdp'), 'tp'), may hold values from -0.078125 to 0.078125
Outputs:
- context: bfloat16 [4096, 5120], P(('fsdp', 'rep'), 'tp')
- policy_key_tp: bfloat16 [5120, 1024], P(None, 'tp')
The draws below stay inside these ranges and needn't reach their ends.
All inputs are finite; a program needn't handle non-finite values.
Results may differ from the reference program's by a relative error of at most 0.0093.
Values may be sent and summed in bfloat16 or wider, within the bound.
A program may use at most 128 MiB of HBM per device.

```python
import math
import jax
import jax.numpy as jnp
import numpy as np
from jax import lax

D = 5120
QH = 40
KVH = 8
HD = 128
TOK_DEV = 1024
TOKENS = 4096
N_FSDP = 4


def draw_ref_bias(key, part):
    width = (QH + 2 * KVH) * HD
    return jnp.clip(0.5 * jax.random.normal(key, (width,), jnp.float32), -3.0, 3.0)


def steps_of(own_key, dims, cuts, least, top_value):
    def one(position, parts):
        steps = jax.random.uniform(jax.random.fold_in(jax.random.fold_in(own_key, 6), position), (parts,), jnp.float32, least / len(cuts), top_value / len(cuts))
        return jnp.repeat(jnp.exp(steps), dims[position] // parts).reshape((-1,) + (1,) * (len(dims) - position - 1))

    level = one(*cuts[0])
    for cut in cuts[1:]:
        level = level * one(*cut)
    return level


def profile(amount, total, bound, skew):
    portions = [(1 << 20) // math.isqrt(rank ** skew) + 1 for rank in range(2, amount + 1)]
    spare, counts = total - bound - (amount - 1), [1] * (amount - 1)
    while spare > 0:
        free = [i for i in range(amount - 1) if counts[i] < bound]
        mass, remaining = sum([portions[i] for i in free]), spare
        for i in free:
            extra = min(bound - counts[i], max(1, remaining * portions[i] // mass), spare)
            counts[i] = counts[i] + extra
            spare = spare - extra
    return np.array([bound] + counts)


def ragged(rng, number_of, total, bound, slope):
    if number_of == 2:
        one = jax.random.randint(rng, (), max(1, total - bound), min(bound, total - 1) + 1)
        return jnp.stack([one, total - one])
    tallies = jnp.asarray(profile(number_of, total, bound, slope), jnp.int32)
    pairs = (number_of - 1) // 2
    giver, sink = tallies[1:1 + 2 * pairs:2], tallies[2:2 + 2 * pairs:2]
    room = jnp.minimum(giver - 1, bound - sink)
    shifted = jax.random.randint(jax.random.fold_in(rng, 1), (pairs,), 0, 1 << 20) % (room + 1)
    tallies = tallies.at[1:1 + 2 * pairs:2].set(giver - shifted).at[2:2 + 2 * pairs:2].set(sink + shifted)
    return tallies[jax.random.permutation(jax.random.fold_in(rng, 2), number_of)]


def noise(own_key, extent, spread, most, pieces=(), kind=jnp.bfloat16):
    result = spread * jax.random.normal(own_key, extent, jnp.float32)
    if pieces:
        result = result * steps_of(own_key, extent, pieces, -0.22, 0.18)
    return jnp.clip(result, -most, most).astype(kind)


def setup_inputs(seed: int = 0) -> dict:
    splits = jax.random.split(jax.random.key(seed), 6)
    tokens = noise(splits[0], (TOKENS, D), 1.0, 6.0, ((0, 4), (1, 4)))
    ref_qkv = noise(splits[1], (D, (QH + 2 * KVH) * HD), D ** -0.5, 0.078125, ((0, 16), (1, 2)))
    ref_bias = draw_ref_bias(jax.random.fold_in(splits[5], 71), 0)
    segment_ids = jax.vmap(lambda own: jnp.searchsorted(jnp.cumsum(ragged(own, max(3, TOK_DEV // 128), TOK_DEV, TOK_DEV // 2, 2)), jnp.arange(TOK_DEV), side="right"))(jax.random.split(splits[3], N_FSDP)).reshape((N_FSDP, TOK_DEV)).astype(jnp.int32)
    policy_key = noise(splits[4], (D, KVH * HD), D ** -0.5, 0.078125, ((0, 16), (1, 2)))
    return {"tokens": tokens, "ref_qkv": ref_qkv, "ref_bias": ref_bias, "segment_ids": segment_ids, "policy_key": policy_key}


def positions_of(seg):
    count = seg.shape[0]
    index = jnp.arange(count, dtype=jnp.int32)
    starts = jnp.concatenate([jnp.ones((1,), bool), seg[1:] != seg[:-1]])
    first = lax.cummax(jnp.where(starts, index, 0).astype(jnp.int32), axis=0)
    return (index - first).astype(jnp.int32)

def rotary(values, pos):
    half = values.shape[-1] // 2
    freq = 1000000.0 ** (-2.0 * jnp.arange(half, dtype=jnp.float32) / values.shape[-1])
    angle = pos.astype(jnp.float32)[:, None] * freq[None, :]
    shape = (values.shape[0],) + (1,) * (values.ndim - 2) + (half,)
    cosine = jnp.cos(angle).reshape(shape)
    sine = jnp.sin(angle).reshape(shape)
    first = values[..., :half]
    second = values[..., half:]
    return jnp.concatenate([first * cosine - second * sine, second * cosine + first * sine], axis=-1)

def reference(tokens, ref_qkv, ref_bias, segment_ids, policy_key):
    share = QH // KVH
    proj = jnp.dot(tokens, ref_qkv, preferred_element_type=jnp.float32) + ref_bias[None, :]
    proj = proj.reshape(N_FSDP, TOK_DEV, KVH, share + 2, HD)

    def one_pack(args):
        block, seg = args
        pos = positions_of(seg)
        query = rotary(block[:, :, :share], pos).astype(jnp.bfloat16)
        keys = rotary(block[:, :, share], pos).astype(jnp.bfloat16)
        vals = block[:, :, share + 1].astype(jnp.bfloat16)
        scores = jnp.einsum('qhgd,khd->hgqk', query.astype(jnp.float32), keys.astype(jnp.float32)) / jnp.sqrt(jnp.float32(HD))
        index = jnp.arange(TOK_DEV)
        allowed = (seg[:, None] == seg[None, :]) & (index[None, :] <= index[:, None])
        scores = jnp.where(allowed[None, None], scores, -1e+30)
        top = lax.optimization_barrier(jnp.max(scores, axis=-1, keepdims=True))
        expo = jnp.exp(scores - top)
        weights = (expo / lax.optimization_barrier(jnp.sum(expo, axis=-1, keepdims=True))).astype(jnp.bfloat16)
        ctx = jnp.einsum('hgqk,khd->qhgd', weights.astype(jnp.float32), vals.astype(jnp.float32))
        return ctx.astype(jnp.bfloat16).reshape(TOK_DEV, QH * HD)
    context = lax.map(one_pack, (proj, segment_ids))
    return (context.reshape(TOKENS, QH * HD), policy_key)
```

```python
import jax
import jax.numpy as jnp
from jax import lax
from jax.experimental import pallas as pl
from jax.experimental.pallas import tpu as pltpu
from jax.sharding import PartitionSpec as P
import functools
import math

MESH = pl.DeviceIdType.MESH

QH = 40
KVH = 8
HD = 128


def positions_of(seg):
    count = seg.shape[0]
    index = jnp.arange(count, dtype=jnp.int32)
    starts = jnp.concatenate([jnp.ones((1,), bool), seg[1:] != seg[:-1]])
    first = lax.cummax(jnp.where(starts, index, 0), axis=0)
    return index - first


def rotary(values, pos):
    half = values.shape[-1] // 2
    freq = 1000000.0 ** (-2.0 * jnp.arange(half, dtype=jnp.float32) / values.shape[-1])
    angle = pos.astype(jnp.float32)[:, None] * freq[None, :]
    shape = (values.shape[0],) + (1,) * (values.ndim - 2) + (half,)
    cosine = jnp.cos(angle).reshape(shape)
    sine = jnp.sin(angle).reshape(shape)
    first = values[..., :half]
    second = values[..., half:]
    return jnp.concatenate(
        [first * cosine - second * sine, second * cosine + first * sine], axis=-1
    )


def per_device(tokens, ref_qkv, ref_bias, segment_ids, policy_key):
    share = QH // KVH
    rows = tokens.shape[0]
    columns = ref_qkv.shape[1]
    groups = columns // ((share + 2) * HD)
    replicas = lax.axis_size("rep")
    mine = rows // replicas
    rank = lax.axis_index("rep")
    partial_value = jnp.dot(
        tokens,
        lax.all_gather(ref_qkv, "fsdp", axis=0, tiled=True),
        preferred_element_type=jnp.float32,
    )
    partial_value = partial_value.reshape(rows, groups, share + 2, HD)
    bias = ref_bias.reshape(groups, share + 2, HD)
    seg = segment_ids[0]
    pos = positions_of(seg)
    start = rank * mine
    my_pos = lax.dynamic_slice_in_dim(pos, start, mine, 0)
    summed = lax.psum_scatter(partial_value, "rep", scatter_dimension=0, tiled=True) + bias[None]
    query = rotary(summed[:, :, :share], my_pos).astype(jnp.bfloat16)
    my_keys = rotary(summed[:, :, share], my_pos).astype(jnp.bfloat16)
    my_vals = summed[:, :, share + 1].astype(jnp.bfloat16)
    keys, vals = (
        lax.all_gather(my_keys, "rep", axis=0, tiled=True),
        lax.all_gather(my_vals, "rep", axis=0, tiled=True),
    )
    scores = jnp.einsum(
        "qhgd,khd->hgqk", query, keys, preferred_element_type=jnp.float32
    ) / jnp.sqrt(jnp.float32(HD))
    query_index = start + jnp.arange(mine, dtype=jnp.int32)
    key_index = jnp.arange(rows, dtype=jnp.int32)
    my_seg = lax.dynamic_slice_in_dim(seg, start, mine, 0)
    allowed = (my_seg[:, None] == seg[None, :]) & (key_index[None, :] <= query_index[:, None])
    scores = jnp.where(allowed[None, None], scores, -1e30)
    top = jnp.max(scores, axis=-1, keepdims=True)
    expo = jnp.exp(scores - top)
    weights = (expo / jnp.sum(expo, axis=-1, keepdims=True)).astype(jnp.bfloat16)
    context = jnp.einsum("hgqk,khd->qhgd", weights, vals, preferred_element_type=jnp.float32)
    context = context.astype(jnp.bfloat16).reshape(mine, groups * share * HD)
    inner = lax.all_gather(policy_key, "rep", axis=0, tiled=True)
    outer = lax.all_gather(inner, "fsdp", axis=0, tiled=True)
    blocks = policy_key.shape[0]
    shards = outer.shape[0] // (blocks * replicas)
    whole = (
        outer.reshape(shards, replicas, blocks, outer.shape[1])
        .transpose(1, 0, 2, 3)
        .reshape(outer.shape)
    )
    return (context, whole)


def greet(devices, extra, condition):
    barrier = pltpu.get_barrier_semaphore()
    for device in devices:
        pl.semaphore_signal(barrier, inc=1, device_id=device, device_id_type=MESH)

    @pl.when(condition)
    def _():
        pl.semaphore_signal(barrier, inc=1, device_id=extra, device_id_type=MESH)
        pl.semaphore_wait(barrier, len(devices) + 1)

    @pl.when(jnp.logical_not(condition))
    def _():
        pl.semaphore_wait(barrier, len(devices))


class Copies:
    def __init__(self, send, recv):
        self.send, self.recv, self.made = send, recv, []

    def make(self, src, dst, device, sends=None):
        n = len(self.made)
        copy = pltpu.make_async_remote_copy(
            src_ref=src, dst_ref=dst, send_sem=self.send.at[n], recv_sem=self.recv.at[n],
            device_id=device, device_id_type=MESH,
        )
        self.made.append((copy, sends))
        return copy

    def start(self, src, dst, device, sends=None):
        copy = self.make(src, dst, device, sends)
        only(sends, copy.start)
        return copy

    def finish(self):
        for copy, sends in self.made:
            only(sends, copy.wait_send)


def only(condition, act):
    if condition is None:
        act()
    else:
        pl.when(condition)(act)


N_COPIES = 62


def layer_kernel(
    tok, w, bias, freq, seg, pol, out, pg,
    x, wg, own, snd, inb, kv, shut, cosine, sine, ctx, pv,
    send, recv, w_local, local, z_send, z_recv,
):
    f, r, t = lax.axis_index("fsdp"), lax.axis_index("rep"), lax.axis_index("tp")
    mine = x.shape[0] // 4
    block, columns = w.shape
    hb = block // 2
    groups = columns // ((QH // KVH + 2) * HD)
    share = QH // KVH
    width = columns // groups
    fx = f + 1 - 2 * lax.rem(f, 2)
    fy = lax.rem(f + 2, 4)
    near = r + 1 - 2 * lax.rem(r, 2)
    across = 3 - r
    end = (r == 0) | (r == 3)
    mid = (r == 1) | (r == 2)
    to_x, to_y, to_near, to_across = {"fsdp": fx}, {"fsdp": fy}, {"rep": near}, {"rep": across}
    to_up, to_down = {"rep": lax.rem(r + 1, 4)}, {"rep": lax.rem(r + 3, 4)}
    copies = Copies(send, recv)

    chunks = [(g * width + share * HD, 2 * HD) for g in range(groups)]
    chunks += [(g * width, share * HD) for g in range(groups)]
    n = len(chunks)
    col = [pl.ds(at, wide) for at, wide in chunks]

    load_w = []
    my_rows = pl.ds(pl.multiple_of(f * block, 16), block)
    for c in range(n):
        load_w.append(pltpu.make_async_copy(w.at[:, col[c]], wg.at[my_rows, col[c]], w_local.at[c]))
        load_w[c].start()
    load_x = pltpu.make_async_copy(tok, x, local.at[0])
    load_p = pltpu.make_async_copy(pol, pv, local.at[1])
    load_p.start()
    load_x.start()
    greet([to_x, to_y, to_near], to_across, mid)

    def held(owner, first, count, c):
        return wg.at[pl.ds(pl.multiple_of(owner * block + first, 16), count), col[c]]

    passed, onwards = {}, {}

    def direct(c):
        load_w[c].wait()
        src = held(f, 0, block, c)
        passed[c] = copies.start(src, src, to_x), copies.start(src, src, to_y)

    def onward(c):
        bx, by = passed[c]
        bx.wait_recv()
        a = copies.start(held(fx, 0, hb, c), held(fx, 0, hb, c), to_y)
        by.wait_recv()
        b = copies.start(held(fy, hb, hb, c), held(fy, hb, hb, c), to_x)
        onwards[c] = a, b

    p_up, p_down = {}, {}

    def policy_z(k):
        up_block, down_block = lax.rem(r + 5 - k, 4), lax.rem(r + k - 1, 4)
        up_src = pv if k == 1 else pg.at[up_block, f]
        down_src = pv if k == 1 else pg.at[down_block, f]
        if k > 1:
            landed_z(k - 1)
        p_up[k] = copies.start(up_src, pg.at[up_block, f], to_up, (r <= 2) & (r >= k - 1))
        p_down[k] = copies.start(down_src, pg.at[down_block, f], to_down, (r >= 1) & (r <= 4 - k))

    def landed_z(k):
        only(r >= k, p_up[k].wait_recv)
        only(r <= 3 - k, p_down[k].wait_recv)

    p_direct, p_onward = {}, {}

    def policy_direct(j):
        src = pg.at[j, f]
        p_direct[j] = copies.start(src, src, to_x), copies.start(src, src, to_y)

    def policy_onward(j):
        top, low = pl.ds(0, hb), pl.ds(hb, hb)
        bx, by = p_direct[j]
        bx.wait_recv()
        a = copies.start(pg.at[j, fx, top], pg.at[j, fx, top], to_y)
        by.wait_recv()
        b = copies.start(pg.at[j, fy, low], pg.at[j, fy, low], to_x)
        p_onward[j] = a, b

    def rows_of(slot):
        ahead = jnp.where(
            slot == 0, 3, jnp.where(slot == 1, 2, jnp.where((slot == 2) == end, 1, 0))
        )
        return jnp.where(r >= 2, 3 - ahead, ahead)

    def partial(c):
        def one(slot, _):
            rows = pl.ds(pl.multiple_of(rows_of(slot) * mine, mine), mine)
            own[slot, :, col[c]] = jnp.dot(x[rows, :], wg[:, col[c]], preferred_element_type=jnp.float32)
            return 0

        lax.fori_loop(0, 4, one, 0)

    def hop(c, slot, place, device):
        return pltpu.make_async_remote_copy(
            src_ref=snd.at[slot, :, col[c]], dst_ref=inb.at[place, :, col[c]],
            send_sem=z_send.at[slot, c], recv_sem=z_recv.at[place, c],
            device_id=device, device_id_type=MESH,
        )

    def came(c, place):
        hop(c, 0, place, to_near).wait_recv()

    def send_from_end(c):
        for slot in range(3):
            snd[slot, :, col[c]] = own[slot, :, col[c]].astype(jnp.bfloat16)
            hop(c, slot, slot, to_near).start()

    def send_from_mid(c):
        for slot, source, place, device in ((0, 0, 3, to_across), (2, 3, 2, to_near), (1, 1, 4, to_across)):
            came(c, source)
            total = own[slot, :, col[c]] + inb[source, :, col[c]].astype(jnp.float32)
            snd[slot, :, col[c]] = total.astype(jnp.bfloat16)
            hop(c, slot, place, device).start()

    def arrive(c):
        came(c, 2)
        pl.when(mid)(lambda: came(c, 4))

    def summed(at):
        return (
            own[3, :, at] + inb[2, :, at].astype(jnp.float32)
            + inb[4, :, at].astype(jnp.float32) + bias[:, at]
        )

    def rotated(values):
        return values * cosine[...] + pltpu.roll(values, HD // 2, 1) * sine[...]

    kv_up, kv_on = {}, {}

    def key_columns(g):
        return pl.ds(g * 2 * HD, HD), pl.ds(g * 2 * HD + HD, HD), pl.ds(g * 2 * HD, 2 * HD)

    def finish_keys(g):
        arrive(g)
        at, _ = chunks[g]
        kc, vc, both = key_columns(g)
        kv[pl.ds(2 * mine, mine), kc] = rotated(summed(pl.ds(at, HD))).astype(jnp.bfloat16)
        kv[pl.ds(2 * mine, mine), vc] = summed(pl.ds(at + HD, HD)).astype(jnp.bfloat16)
        kv_up[g] = copies.start(
            kv.at[pl.ds(2 * mine, mine), both], kv.at[pl.ds(mine, mine), both], to_up, r <= 2
        )

    def forward_keys(g):
        _, _, both = key_columns(g)
        only(r >= 1, kv_up[g].wait_recv)
        kv_on[g] = copies.start(
            kv.at[pl.ds(mine, mine), both], kv.at[pl.ds(0, mine), both], to_up, mid
        )

    scale = 1.0 / math.sqrt(HD)
    outs = []

    def attend(g):
        c = groups + g
        arrive(c)
        only(r >= 2, kv_on[g].wait_recv)
        kc, vc, _ = key_columns(g)

        def head(j, _):
            at = pl.ds(pl.multiple_of(g * width + j * HD, HD), HD)
            query = rotated(summed(at)).astype(jnp.bfloat16)
            scores = lax.dot_general(
                query, kv[:, kc], (((1,), (1,)), ((), ())), preferred_element_type=jnp.float32
            ) * scale + shut[...]
            expo = jnp.exp(scores - jnp.max(scores, axis=-1, keepdims=True))
            total = jnp.sum(expo, axis=-1, keepdims=True)
            weights = (expo * (1.0 / total)).astype(jnp.bfloat16)
            to = pl.ds(pl.multiple_of((g * share + j) * HD, HD), HD)
            ctx[:, to] = jnp.dot(weights, kv[:, vc], preferred_element_type=jnp.float32).astype(jnp.bfloat16)
            return 0

        lax.fori_loop(0, share, head, 0)
        part = pl.ds(g * share * HD, share * HD)
        copy = pltpu.make_async_copy(ctx.at[:, part], out.at[:, part], local.at[3 + g])
        copy.start()
        outs.append(copy)

    def prepare():
        at = pl.ds(pl.multiple_of(r * mine, mine), mine)
        square = (mine, mine)
        row, lane = lax.broadcasted_iota(jnp.int32, square, 0), lax.broadcasted_iota(jnp.int32, square, 1)
        mine_row = jnp.broadcast_to(seg[:, at].astype(jnp.float32), square)
        my_seg = jnp.sum(jnp.where(row == lane, mine_row, 0.0), axis=-1, keepdims=True)
        before = jnp.where(seg[...].astype(jnp.float32) < my_seg, 1.0, 0.0)
        first = jnp.sum(before, axis=-1, keepdims=True)
        index = lax.broadcasted_iota(jnp.int32, (mine, HD), 0) + r * mine
        angle = (index.astype(jnp.float32) - first) * freq[...]
        half = lax.broadcasted_iota(jnp.int32, (mine, HD), 1) < HD // 2
        cosine[...] = jnp.cos(angle)
        wave = jnp.sin(angle)
        sine[...] = jnp.where(half, -wave, wave)
        for slot in range(3):
            there = r - 2 + slot
            keys = pl.ds(pl.multiple_of(jnp.maximum(there, 0) * mine, mine), mine)
            allowed = (my_seg == seg[:, keys].astype(jnp.float32)) & (there >= 0)
            if slot == 2:
                allowed = allowed & (lane <= row)
            shut[:, slot * mine:(slot + 1) * mine] = jnp.where(allowed, 0.0, -1e30)

        @pl.when(r <= 1)
        def _():
            kv[pl.ds(0, mine), :] = jnp.zeros((mine, kv.shape[1]), kv.dtype)

        @pl.when(r == 0)
        def _():
            kv[pl.ds(mine, mine), :] = jnp.zeros((mine, kv.shape[1]), kv.dtype)

        @pl.when(end)
        def _():
            inb[4] = jnp.zeros(inb.shape[1:], inb.dtype)

    direct(0)
    direct(1)
    load_p.wait()
    policy_z(1)
    keep_p = pltpu.make_async_copy(pv, pg.at[r, f], local.at[2])
    keep_p.start()
    onward(0)
    direct(2)
    onward(1)
    direct(3)
    load_x.wait()
    for c in range(n):
        for copy in onwards[c]:
            copy.wait_recv()
        partial(c)
        pl.when(end)(functools.partial(send_from_end, c))
        if c + 2 < n:
            onward(c + 2)
        if c + 4 < n:
            direct(c + 4)
        if c == 0:
            prepare()
            policy_z(2)
        if c == 1:
            policy_z(3)
        if c == 4:
            landed_z(3)
            keep_p.wait()
            policy_direct(0)
            policy_direct(1)
        if c == 6:
            policy_onward(0)
            policy_direct(2)
            policy_onward(1)
            policy_direct(3)
        pl.when(mid)(functools.partial(send_from_mid, c))
        if c == groups + 1:
            for g in range(groups):
                forward_keys(g)
        if 1 <= c <= groups:
            finish_keys(c - 1)
        if c > groups:
            attend(c - 1 - groups)
    policy_onward(2)
    policy_onward(3)
    attend(groups - 1)
    for copy in outs:
        copy.wait()
    for j in range(4):
        for copy in p_onward[j]:
            copy.wait_recv()
    for c in range(n):
        for slot in range(3):
            hop(c, slot, 0, to_near).wait_send()
    copies.finish()


def whole_layer(tokens, ref_qkv, ref_bias, segment_ids, policy_key):
    rows, depth = tokens.shape
    block, columns = ref_qkv.shape
    mine, share = rows // 4, QH // KVH
    groups = columns // ((share + 2) * HD)
    chunks = 2 * groups
    half = HD // 2
    freq = 1000000.0 ** (-2.0 * jnp.arange(half, dtype=jnp.float32) / HD)
    freq = jnp.concatenate([freq, freq])[None, :]
    any_space, vmem = pl.BlockSpec(memory_space=pl.ANY), pl.BlockSpec(memory_space=pltpu.VMEM)
    low, full = jnp.bfloat16, jnp.float32
    dma = pltpu.SemaphoreType.DMA
    out, pg = pl.pallas_call(
        layer_kernel,
        out_shape=(
            jax.ShapeDtypeStruct((mine, groups * share * HD), low),
            jax.ShapeDtypeStruct((4, 4) + policy_key.shape, policy_key.dtype),
        ),
        in_specs=[any_space, any_space, vmem, vmem, vmem, any_space],
        out_specs=(any_space, any_space),
        scratch_shapes=[
            pltpu.VMEM((rows, depth), tokens.dtype),
            pltpu.VMEM((4 * block, columns), ref_qkv.dtype),
            pltpu.VMEM((4, mine, columns), full),
            pltpu.VMEM((3, mine, columns), low),
            pltpu.VMEM((5, mine, columns), low),
            pltpu.VMEM((3 * mine, groups * 2 * HD), low),
            pltpu.VMEM((mine, 3 * mine), full),
            pltpu.VMEM((mine, HD), full),
            pltpu.VMEM((mine, HD), full),
            pltpu.VMEM((mine, groups * share * HD), low),
            pltpu.VMEM(policy_key.shape, policy_key.dtype),
            dma((N_COPIES,)),
            dma((N_COPIES,)),
            dma((chunks,)),
            dma((3 + groups,)),
            dma((3, chunks)),
            dma((5, chunks)),
        ],
        compiler_params=pltpu.CompilerParams(
            collective_id=0, has_side_effects=True, vmem_limit_bytes=60 * 1024 * 1024
        ),
    )(tokens, ref_qkv, ref_bias[None, :], freq, segment_ids, policy_key)
    return out, pg.reshape((-1,) + policy_key.shape[1:])


def solution(mesh):
    in_specs = (
        P("fsdp", "rep"),
        P(("rep", "fsdp"), "tp"),
        P("tp"),
        P("fsdp", None),
        P(("rep", "fsdp"), "tp"),
    )
    out_specs = (P(("fsdp", "rep"), "tp"), P(None, "tp"))
    shape = mesh.shape
    grouped = shape["rep"] == 4 and shape["fsdp"] == 4 and shape["tp"] == 2
    return jax.shard_map(
        whole_layer if grouped else per_device, mesh=mesh, in_specs=in_specs, out_specs=out_specs, check_vma=False
    )
```

```python
import jax
import jax.numpy as jnp
from jax import lax
from jax.experimental import pallas as pl
from jax.experimental.pallas import tpu as pltpu
from jax.sharding import PartitionSpec as P
import functools
import math

MESH = pl.DeviceIdType.MESH

QH = 40
KVH = 8
HD = 128


def positions_of(seg):
    count = seg.shape[0]
    index = jnp.arange(count, dtype=jnp.int32)
    starts = jnp.concatenate([jnp.ones((1,), bool), seg[1:] != seg[:-1]])
    first = lax.cummax(jnp.where(starts, index, 0), axis=0)
    return index - first


def rotary(values, pos):
    half = values.shape[-1] // 2
    freq = 1000000.0 ** (-2.0 * jnp.arange(half, dtype=jnp.float32) / values.shape[-1])
    angle = pos.astype(jnp.float32)[:, None] * freq[None, :]
    shape = (values.shape[0],) + (1,) * (values.ndim - 2) + (half,)
    cosine = jnp.cos(angle).reshape(shape)
    sine = jnp.sin(angle).reshape(shape)
    first = values[..., :half]
    second = values[..., half:]
    return jnp.concatenate(
        [first * cosine - second * sine, second * cosine + first * sine], axis=-1
    )


def per_device(tokens, ref_qkv, ref_bias, segment_ids, policy_key):
    share = QH // KVH
    rows = tokens.shape[0]
    columns = ref_qkv.shape[1]
    groups = columns // ((share + 2) * HD)
    replicas = lax.axis_size("rep")
    mine = rows // replicas
    rank = lax.axis_index("rep")
    partial_value = jnp.dot(
        tokens,
        lax.all_gather(ref_qkv, "fsdp", axis=0, tiled=True),
        preferred_element_type=jnp.float32,
    )
    partial_value = partial_value.reshape(rows, groups, share + 2, HD)
    bias = ref_bias.reshape(groups, share + 2, HD)
    seg = segment_ids[0]
    pos = positions_of(seg)
    start = rank * mine
    my_pos = lax.dynamic_slice_in_dim(pos, start, mine, 0)
    summed = lax.psum_scatter(partial_value, "rep", scatter_dimension=0, tiled=True) + bias[None]
    query = rotary(summed[:, :, :share], my_pos).astype(jnp.bfloat16)
    my_keys = rotary(summed[:, :, share], my_pos).astype(jnp.bfloat16)
    my_vals = summed[:, :, share + 1].astype(jnp.bfloat16)
    keys, vals = (
        lax.all_gather(my_keys, "rep", axis=0, tiled=True),
        lax.all_gather(my_vals, "rep", axis=0, tiled=True),
    )
    scores = jnp.einsum(
        "qhgd,khd->hgqk", query, keys, preferred_element_type=jnp.float32
    ) / jnp.sqrt(jnp.float32(HD))
    query_index = start + jnp.arange(mine, dtype=jnp.int32)
    key_index = jnp.arange(rows, dtype=jnp.int32)
    my_seg = lax.dynamic_slice_in_dim(seg, start, mine, 0)
    allowed = (my_seg[:, None] == seg[None, :]) & (key_index[None, :] <= query_index[:, None])
    scores = jnp.where(allowed[None, None], scores, -1e30)
    top = jnp.max(scores, axis=-1, keepdims=True)
    expo = jnp.exp(scores - top)
    weights = (expo / jnp.sum(expo, axis=-1, keepdims=True)).astype(jnp.bfloat16)
    context = jnp.einsum("hgqk,khd->qhgd", weights, vals, preferred_element_type=jnp.float32)
    context = context.astype(jnp.bfloat16).reshape(mine, groups * share * HD)
    inner = lax.all_gather(policy_key, "rep", axis=0, tiled=True)
    outer = lax.all_gather(inner, "fsdp", axis=0, tiled=True)
    blocks = policy_key.shape[0]
    shards = outer.shape[0] // (blocks * replicas)
    whole = (
        outer.reshape(shards, replicas, blocks, outer.shape[1])
        .transpose(1, 0, 2, 3)
        .reshape(outer.shape)
    )
    return (context, whole)


def greet(devices, extra, condition):
    barrier = pltpu.get_barrier_semaphore()
    for device in devices:
        pl.semaphore_signal(barrier, inc=1, device_id=device, device_id_type=MESH)

    @pl.when(condition)
    def _():
        pl.semaphore_signal(barrier, inc=1, device_id=extra, device_id_type=MESH)
        pl.semaphore_wait(barrier, len(devices) + 1)

    @pl.when(jnp.logical_not(condition))
    def _():
        pl.semaphore_wait(barrier, len(devices))


class Copies:
    def __init__(self, send, recv, ring):
        self.send, self.recv, self.ring = send, recv, ring
        self.made, self.done, self.left, self.used = [], 0, set(), 0

    def place(self):
        self.used += 1
        return self.used - 1

    def start(self, src, dst, device, sends=None, place=None):
        n = len(self.made)
        self.retire(n - self.ring + 1)
        place = self.place() if place is None else place
        copy = pltpu.make_async_remote_copy(
            src_ref=src, dst_ref=dst, send_sem=self.send.at[n % self.ring], recv_sem=self.recv.at[place],
            device_id=device, device_id_type=MESH,
        )
        only(sends, copy.start)
        self.made.append((copy, sends))
        return copy

    def arrival(self, ref, device, place):
        return pltpu.make_async_remote_copy(
            src_ref=ref, dst_ref=ref, send_sem=self.send.at[0], recv_sem=self.recv.at[place],
            device_id=device, device_id_type=MESH,
        )

    def sent(self, n):
        if n not in self.left:
            self.left.add(n)
            copy, sends = self.made[n]
            only(sends, copy.wait_send)

    def retire(self, count):
        while self.done < count:
            self.sent(self.done)
            self.done += 1


def only(condition, act):
    if condition is None:
        act()
    else:
        pl.when(condition)(act)


def sizes_of(g, groups, share):
    if g == groups - 1:
        return [2] * (share // 2) + [1] * (share % 2)
    return [share - share // 2, share // 2]


def plan(groups, share):
    width = (share + 2) * HD
    pieces = []
    for g in range(groups):
        pair = [("k", g, share), ("v", g, share + 1)]
        pieces += [pair[:1], pair[1:]] if g == 0 else [pair]
    for g in range(groups):
        at = 0
        for size in sizes_of(g, groups, share):
            pieces.append([("q", g, j) for j in range(at, at + size)])
            at += size
    return [(heads[0][1] * width + heads[0][2] * HD, heads) for heads in pieces]


def layer_kernel(
    tok, w, bias, seg, pol, out, pg,
    x, wg, own, fin, snd, inb, kv, shut, cosine, sine, ctx, pv,
    send, recv, w_local, local, z_send, z_recv,
):
    f, r, t = lax.axis_index("fsdp"), lax.axis_index("rep"), lax.axis_index("tp")
    mine = x.shape[0] // 4
    block, columns = w.shape
    hb = block // 2
    share = QH // KVH
    width = (share + 2) * HD
    groups = columns // width
    fx = f + 1 - 2 * lax.rem(f, 2)
    fy = lax.rem(f + 2, 4)
    near = r + 1 - 2 * lax.rem(r, 2)
    across = 3 - r
    end = (r == 0) | (r == 3)
    mid = (r == 1) | (r == 2)
    to_x, to_y, to_near, to_across = {"fsdp": fx}, {"fsdp": fy}, {"rep": near}, {"rep": across}
    to_up, to_down = {"rep": lax.rem(r + 1, 4)}, {"rep": lax.rem(r + 3, 4)}
    copies = Copies(send, recv, RING)

    chunks = plan(groups, share)
    n = len(chunks)
    wide = [len(heads) * HD for _, heads in chunks]
    col = [pl.ds(at, wide[c]) for c, (at, _) in enumerate(chunks)]

    my_rows = pl.ds(pl.multiple_of(f * block, 16), block)
    parts = col[:2] + [pl.ds(width, columns - width), pl.ds(0, share * HD)]
    load_w = [pltpu.make_async_copy(w.at[:, at], wg.at[my_rows, at], w_local.at[i]) for i, at in enumerate(parts)]
    for copy in load_w:
        copy.start()
    loaded = set()
    load_x = pltpu.make_async_copy(tok, x, local.at[0])
    load_p = pltpu.make_async_copy(pol, pv, local.at[1])
    load_p.start()
    load_x.start()
    greet([to_x, to_y, to_near], to_across, mid)

    def held(owner, first, count, c):
        return wg.at[pl.ds(pl.multiple_of(owner * block + first, 16), count), col[c]]

    passed, onwards, last_direct = {}, {}, {}

    def direct(c):
        part = c if c < 2 else (3 if chunks[c][0] < width else 2)
        if part not in loaded:
            loaded.add(part)
            load_w[part].wait()
        src = held(f, 0, block, c)
        place = copies.place()
        last_direct[c] = len(copies.made)
        copies.start(src, src, to_x, place=place)
        copies.start(src, src, to_y, place=place)
        passed[c] = copies.arrival(wg.at[pl.ds(0, 2 * block), col[c]], to_x, place)

    def left(c):
        copies.sent(last_direct[c])
        copies.sent(last_direct[c] + 1)

    def onward(c):
        passed[c].wait_recv()
        place = copies.place()
        copies.start(held(fx, 0, hb, c), held(fx, 0, hb, c), to_y, place=place)
        copies.start(held(fy, hb, hb, c), held(fy, hb, hb, c), to_x, place=place)
        onwards[c] = copies.arrival(wg.at[pl.ds(0, block), col[c]], to_x, place)

    def policy_at(j, owner, first=0, count=block):
        return pg.at[pl.ds(pl.multiple_of((j * 4 + owner) * block + first, 16), count)]

    p_up, p_down = {}, {}

    def policy_z(k):
        up_block, down_block = lax.rem(r + 5 - k, 4), lax.rem(r + k - 1, 4)
        up_src = pv if k == 1 else policy_at(up_block, f)
        down_src = pv if k == 1 else policy_at(down_block, f)
        if k > 1:
            landed_z(k - 1)
        p_up[k] = copies.start(up_src, policy_at(up_block, f), to_up, (r <= 2) & (r >= k - 1))
        p_down[k] = copies.start(down_src, policy_at(down_block, f), to_down, (r >= 1) & (r <= 4 - k))

    def landed_z(k):
        only(r >= k, p_up[k].wait_recv)
        only(r <= 3 - k, p_down[k].wait_recv)

    p_direct, p_onward = {}, {}

    def policy_direct(j):
        src, place = policy_at(j, f), copies.place()
        copies.start(src, src, to_x, place=place)
        copies.start(src, src, to_y, place=place)
        p_direct[j] = copies.arrival(pg.at[pl.ds(0, 2 * block)], to_x, place)

    def policy_onward(j):
        p_direct[j].wait_recv()
        place = copies.place()
        copies.start(policy_at(j, fx, 0, hb), policy_at(j, fx, 0, hb), to_y, place=place)
        copies.start(policy_at(j, fy, hb, hb), policy_at(j, fy, hb, hb), to_x, place=place)
        p_onward[j] = copies.arrival(pg.at[pl.ds(0, block)], to_x, place)

    def rows_of(slot):
        ahead = jnp.where(
            slot == 0, 3, jnp.where(slot == 1, 2, jnp.where((slot == 2) == end, 1, 0))
        )
        return jnp.where(r >= 2, 3 - ahead, ahead)

    def product(c, slot):
        rows = pl.ds(pl.multiple_of(rows_of(slot) * mine, mine), mine)
        return jnp.dot(x[rows, :], wg[:, col[c]], preferred_element_type=jnp.float32)

    def hop(c, slot, place, device):
        return pltpu.make_async_remote_copy(
            src_ref=snd.at[slot, :, col[c]], dst_ref=inb.at[place, :, col[c]],
            send_sem=z_send.at[slot, c % HOPS], recv_sem=z_recv.at[z_place(place), c],
            device_id=device, device_id_type=MESH,
        )

    def z_place(place):
        return (0, 1, 3, 2, 3)[place]

    def came(c, place):
        hop(c, 0, place, to_near).wait_recv()

    def came_last(c):
        both = inb.at[pl.ds(0, 2), :, col[c]]
        pair = pltpu.make_async_remote_copy(
            src_ref=both, dst_ref=both, send_sem=z_send.at[0, 0], recv_sem=z_recv.at[3, c],
            device_id=to_near, device_id_type=MESH,
        )
        pl.when(mid)(pair.wait_recv)
        pl.when(end)(hop(c, 0, 2, to_near).wait_recv)

    def work_end(c):
        def one(slot, _):
            snd[slot, :, col[c]] = product(c, slot).astype(jnp.bfloat16)
            pltpu.make_async_remote_copy(
                src_ref=snd.at[slot, :, col[c]], dst_ref=inb.at[slot, :, col[c]],
                send_sem=z_send.at[slot, c % HOPS], recv_sem=z_recv.at[jnp.where(slot == 2, 3, slot), c],
                device_id=to_near, device_id_type=MESH,
            ).start()
            return 0

        lax.fori_loop(0, 3, one, 0)
        fin[:, col[c]] = product(c, 3)

    def work_mid(c):
        here = pl.ds(0, wide[c])

        def one(slot, _):
            own[slot_of(c), slot, :, here] = product(c, slot)
            return 0

        lax.fori_loop(0, 3, one, 0)
        fin[:, col[c]] = product(c, 3)

    def work_one(c):
        if c >= 1:
            work_back(c - 1)
        if c == n - 1:
            work_back(c)
        work_across(c)

    def work_two(c):
        work_across(c)
        if c >= 1:
            work_back(c - 1)

    def work_across(c):
        relay(c, 0, 0, 3, to_across)
        relay(c, 1, 1, 4, to_across)

    def relay(c, slot, source, place, device):
        came(c, source)
        total = own[slot_of(c), slot, :, pl.ds(0, wide[c])] + inb[source, :, col[c]].astype(jnp.float32)
        snd[slot, :, col[c]] = total.astype(jnp.bfloat16)
        hop(c, slot, place, device).start()

    def work_back(c):
        relay(c, 2, 3, 2, to_near)

    def slot_of(c):
        return c % 2

    def summed(at):
        return (
            fin[:, at] + inb[2, :, at].astype(jnp.float32)
            + inb[4, :, at].astype(jnp.float32) + bias[at][None, :]
        )

    def rotated(values):
        return values * cosine[...] + pltpu.roll(values, HD // 2, 1) * sine[...]

    kv_up, kv_on = {}, {}

    def stored(kind, g):
        return pl.ds((2 * g + (kind == "v")) * HD, HD)

    def span(c):
        _, heads = chunks[c]
        return pl.ds((2 * heads[0][1] + (heads[0][0] == "v")) * HD, wide[c])

    key_chunks = [c for c in range(n) if chunks[c][1][0][0] != "q"]
    low, middle, high = (pl.ds(k * mine, mine) for k in range(3))

    def finish_keys(c):
        at, heads = chunks[c]
        for kind, g, j in heads:
            values = summed(pl.ds(at + (j - heads[0][2]) * HD, HD))
            kv[high, stored(kind, g)] = (rotated(values) if kind == "k" else values).astype(jnp.bfloat16)
        kv_up[c] = copies.start(kv.at[high, span(c)], kv.at[middle, span(c)], to_up, r <= 2)

    def forward_keys(c):
        only(r >= 1, kv_up[c].wait_recv)
        kv_on[c] = copies.start(kv.at[middle, span(c)], kv.at[low, span(c)], to_up, mid)

    scale = 1.0 / math.sqrt(HD)
    keys_in = set()

    def attend(c):
        at, heads = chunks[c]
        _, g, first = heads[0]
        for k in key_chunks:
            if k not in keys_in and chunks[k][1][0][1] == g:
                keys_in.add(k)
                only(r >= 2, kv_on[k].wait_recv)
        kc, vc = stored("k", g), stored("v", g)
        base = (g * share + first) * HD

        def head(j, _):
            query = rotated(summed(pl.ds(pl.multiple_of(at + j * HD, HD), HD))).astype(jnp.bfloat16)
            scores = lax.dot_general(
                query, kv[:, kc], (((1,), (1,)), ((), ())), preferred_element_type=jnp.float32
            ) * scale + shut[...]
            expo = jnp.exp(scores - jnp.max(scores, axis=-1, keepdims=True))
            total = jnp.sum(expo, axis=-1, keepdims=True)
            weights = (expo * (1.0 / total)).astype(jnp.bfloat16)
            to = pl.ds(pl.multiple_of(base + j * HD, HD), HD)
            ctx[:, to] = jnp.dot(weights, kv[:, vc], preferred_element_type=jnp.float32).astype(jnp.bfloat16)
            return 0

        lax.fori_loop(0, len(heads), head, 0)
        part = pl.ds(base, wide[c])
        pltpu.make_async_copy(ctx.at[:, part], out.at[:, part], local.at[3]).start()

    def finish(c):
        came_last(c)
        (attend if chunks[c][1][0][0] == "q" else finish_keys)(c)

    def prepare():
        at = pl.ds(pl.multiple_of(r * mine, mine), mine)
        square = (mine, mine)
        row, lane = lax.broadcasted_iota(jnp.int32, square, 0), lax.broadcasted_iota(jnp.int32, square, 1)
        mine_row = jnp.broadcast_to(seg[:, at].astype(jnp.float32), square)
        my_seg = jnp.sum(jnp.where(row == lane, mine_row, 0.0), axis=-1, keepdims=True)
        before = jnp.where(seg[...].astype(jnp.float32) < my_seg, 1.0, 0.0)
        first = jnp.sum(before, axis=-1, keepdims=True)
        index = lax.broadcasted_iota(jnp.int32, (mine, HD), 0) + r * mine
        half = HD // 2
        place = lax.rem(lax.broadcasted_iota(jnp.int32, (1, HD), 1), half)
        freq = jnp.ones((1, HD), jnp.float32)
        for i in range(1, half):
            freq = jnp.where(place == i, 1000000.0 ** (-2.0 * i / HD), freq)
        angle = (index.astype(jnp.float32) - first) * freq
        cosine[...] = jnp.cos(angle)
        wave = jnp.sin(angle)
        sine[...] = jnp.where(lax.broadcasted_iota(jnp.int32, (mine, HD), 1) < half, -wave, wave)
        for slot in range(3):
            there = r - 2 + slot
            keys = pl.ds(pl.multiple_of(jnp.maximum(there, 0) * mine, mine), mine)
            allowed = (my_seg == seg[:, keys].astype(jnp.float32)) & (there >= 0)
            if slot == 2:
                allowed = allowed & (lane <= row)
            shut[:, slot * mine:(slot + 1) * mine] = jnp.where(allowed, 0.0, -1e30)

        @pl.when(r <= 1)
        def _():
            kv[low, :] = jnp.zeros((mine, kv.shape[1]), kv.dtype)

        @pl.when(r == 0)
        def _():
            kv[middle, :] = jnp.zeros((mine, kv.shape[1]), kv.dtype)

        @pl.when(end)
        def _():
            inb[4] = jnp.zeros(inb.shape[1:], inb.dtype)

    def weights_in(c):
        onwards[c].wait_recv()

    queries = len(key_chunks)
    direct(0)
    load_p.wait()
    policy_z(1)
    keep_p = pltpu.make_async_copy(pv, policy_at(r, f), local.at[2])
    keep_p.start()
    left(0)
    direct(1)
    onward(0)
    direct(2)
    onward(1)
    direct(3)
    load_x.wait()
    weights_in(0)
    pl.when(end)(functools.partial(work_end, 0))
    onward(2)
    direct(4)
    prepare()
    policy_steps = {
        queries - 1: [("d", 0)], queries: [("d", 1)], queries + 1: [("o", 0), ("d", 2)], queries + 2: [("o", 1)],
        queries + 3: [("d", 3), ("o", 2)], queries + 5: [("o", 3)],
    }

    def weights_on(c):
        if c + 3 < n:
            onward(c + 3)
        if c + 5 < n:
            direct(c + 5)

    def sends_out(c):
        for slot in range(3):
            hop(c, slot, 0, to_near).wait_send()

    for c in range(n):
        if c + 1 >= HOPS:
            sends_out(c + 1 - HOPS)
        if 0 <= c - 4 < queries:
            forward_keys(c - 4)
        early = c - 2 < queries - 2
        if 0 <= c - 2 < queries and not early:
            finish(c - 2)
        if c + 1 < n:
            weights_in(c + 1)
            pl.when(end)(functools.partial(work_end, c + 1))
        if 0 <= c - 2 and early:
            finish(c - 2)
        if c < 3:
            weights_on(c)
        if c == 0:
            policy_z(2)
        if c == 2:
            policy_z(3)
        pl.when(mid)(functools.partial(work_mid, c))
        pl.when(r == 1)(functools.partial(work_one, c))
        pl.when(r == 2)(functools.partial(work_two, c))
        if c >= 3:
            weights_on(c)
        if c == queries - 1:
            landed_z(3)
            keep_p.wait()
        for kind, j in policy_steps.get(c, ()):
            (policy_direct if kind == "d" else policy_onward)(j)
        if queries <= c - 2 < n - 3:
            finish(c - 2)
        if c == n - 2:
            finish(c - 1)
    finish(n - 2)
    pl.when(r == 2)(functools.partial(work_back, n - 1))
    finish(n - 1)
    for j in range(4):
        p_onward[j].wait_recv()
    for c in range(n + 1 - HOPS, n):
        sends_out(c)
    copies.retire(len(copies.made))
    pltpu.make_async_copy(ctx, out, local.at[3]).wait()


def settle_kernel(ctx, pg, out, whole, ctx_held, pg_held, load, store):
    pieces = [(ctx, ctx_held, out, pl.ds(k * 128, 128)) for k in range(ctx.shape[0] // 128)]
    step = pg.shape[0] // 8
    pieces = [(pg, pg_held, whole, pl.ds(k * step, step)) for k in range(8)] + pieces
    loads = [
        pltpu.make_async_copy(src.at[at], held.at[at], load.at[i]) for i, (src, held, _, at) in enumerate(pieces)
    ]
    stores = [
        pltpu.make_async_copy(held.at[at], dst.at[at], store.at[i]) for i, (_, held, dst, at) in enumerate(pieces)
    ]
    for copy in loads:
        copy.start()
    for one, two in zip(loads, stores):
        one.wait()
        two.start()
    for copy in stores:
        copy.wait()


def whole_layer(tokens, ref_qkv, ref_bias, segment_ids, policy_key):
    rows, depth = tokens.shape
    block, columns = ref_qkv.shape
    mine, share = rows // 4, QH // KVH
    groups = columns // ((share + 2) * HD)
    chunks = plan(groups, share)
    n = len(chunks)
    keys = sum(heads[0][0] != "q" for _, heads in chunks)
    widest = max(len(heads) for _, heads in chunks) * HD
    places = 2 * n + 6 + 2 * keys + 8
    hbm, vmem = pl.BlockSpec(memory_space=pltpu.HBM), pl.BlockSpec(memory_space=pltpu.VMEM)
    any_space = pl.BlockSpec(memory_space=pl.ANY)
    low, full = jnp.bfloat16, jnp.float32
    dma = pltpu.SemaphoreType.DMA
    out, pg = pl.pallas_call(
        layer_kernel,
        out_shape=(
            jax.ShapeDtypeStruct((mine, groups * share * HD), low),
            jax.ShapeDtypeStruct((16 * block, policy_key.shape[1]), policy_key.dtype),
        ),
        in_specs=[hbm, hbm, vmem, vmem, hbm],
        out_specs=(any_space, any_space),
        scratch_shapes=[
            pltpu.VMEM((rows, depth), tokens.dtype),
            pltpu.VMEM((4 * block, columns), ref_qkv.dtype),
            pltpu.VMEM((2, 3, mine, widest), full),
            pltpu.VMEM((mine, columns), full),
            pltpu.VMEM((3, mine, columns), low),
            pltpu.VMEM((5, mine, columns), low),
            pltpu.VMEM((3 * mine, groups * 2 * HD), low),
            pltpu.VMEM((mine, 3 * mine), full),
            pltpu.VMEM((mine, HD), full),
            pltpu.VMEM((mine, HD), full),
            pltpu.VMEM((mine, groups * share * HD), low),
            pltpu.VMEM(policy_key.shape, policy_key.dtype),
            dma((RING,)),
            dma((places,)),
            dma((4,)),
            dma((4,)),
            dma((3, HOPS)),
            dma((4, n)),
        ],
        compiler_params=pltpu.CompilerParams(
            collective_id=0, has_side_effects=True, vmem_limit_bytes=VMEM_LIMIT
        ),
    )(tokens, ref_qkv, ref_bias, segment_ids, policy_key)
    pieces = 8 + mine // 128
    return pl.pallas_call(
        settle_kernel,
        out_shape=tuple(jax.ShapeDtypeStruct(a.shape, a.dtype) for a in (out, pg)),
        in_specs=[any_space] * 2,
        out_specs=(any_space,) * 2,
        scratch_shapes=[
            pltpu.VMEM(out.shape, out.dtype), pltpu.VMEM(pg.shape, pg.dtype), dma((pieces,)), dma((pieces,)),
        ],
        compiler_params=pltpu.CompilerParams(vmem_limit_bytes=VMEM_LIMIT),
    )(out, pg)


VMEM_LIMIT = 60 * 1024 * 1024
RING = 32
HOPS = 4


def solution(mesh):
    in_specs = (
        P("fsdp", "rep"),
        P(("rep", "fsdp"), "tp"),
        P("tp"),
        P("fsdp", None),
        P(("rep", "fsdp"), "tp"),
    )
    out_specs = (P(("fsdp", "rep"), "tp"), P(None, "tp"))
    shape = mesh.shape
    grouped = shape["rep"] == 4 and shape["fsdp"] == 4 and shape["tp"] == 2
    return jax.shard_map(
        whole_layer if grouped else per_device, mesh=mesh, in_specs=in_specs, out_specs=out_specs, check_vma=False
    )
```

```python
import jax
import jax.numpy as jnp
from jax import lax
from jax.experimental import pallas as pl
from jax.experimental.pallas import tpu as pltpu
from jax.sharding import PartitionSpec as P
import functools
import math

MESH = pl.DeviceIdType.MESH

QH = 40
KVH = 8
HD = 128


def positions_of(seg):
    count = seg.shape[0]
    index = jnp.arange(count, dtype=jnp.int32)
    starts = jnp.concatenate([jnp.ones((1,), bool), seg[1:] != seg[:-1]])
    first = lax.cummax(jnp.where(starts, index, 0), axis=0)
    return index - first


def rotary(values, pos):
    half = values.shape[-1] // 2
    freq = 1000000.0 ** (-2.0 * jnp.arange(half, dtype=jnp.float32) / values.shape[-1])
    angle = pos.astype(jnp.float32)[:, None] * freq[None, :]
    shape = (values.shape[0],) + (1,) * (values.ndim - 2) + (half,)
    cosine = jnp.cos(angle).reshape(shape)
    sine = jnp.sin(angle).reshape(shape)
    first = values[..., :half]
    second = values[..., half:]
    return jnp.concatenate(
        [first * cosine - second * sine, second * cosine + first * sine], axis=-1
    )


def per_device(tokens, ref_qkv, ref_bias, segment_ids, policy_key):
    share = QH // KVH
    rows = tokens.shape[0]
    columns = ref_qkv.shape[1]
    groups = columns // ((share + 2) * HD)
    replicas = lax.axis_size("rep")
    mine = rows // replicas
    rank = lax.axis_index("rep")
    partial_value = jnp.dot(
        tokens,
        lax.all_gather(ref_qkv, "fsdp", axis=0, tiled=True),
        preferred_element_type=jnp.float32,
    )
    partial_value = partial_value.reshape(rows, groups, share + 2, HD)
    bias = ref_bias.reshape(groups, share + 2, HD)
    seg = segment_ids[0]
    pos = positions_of(seg)
    start = rank * mine
    my_pos = lax.dynamic_slice_in_dim(pos, start, mine, 0)
    summed = lax.psum_scatter(partial_value, "rep", scatter_dimension=0, tiled=True) + bias[None]
    query = rotary(summed[:, :, :share], my_pos).astype(jnp.bfloat16)
    my_keys = rotary(summed[:, :, share], my_pos).astype(jnp.bfloat16)
    my_vals = summed[:, :, share + 1].astype(jnp.bfloat16)
    keys, vals = (
        lax.all_gather(my_keys, "rep", axis=0, tiled=True),
        lax.all_gather(my_vals, "rep", axis=0, tiled=True),
    )
    scores = jnp.einsum(
        "qhgd,khd->hgqk", query, keys, preferred_element_type=jnp.float32
    ) / jnp.sqrt(jnp.float32(HD))
    query_index = start + jnp.arange(mine, dtype=jnp.int32)
    key_index = jnp.arange(rows, dtype=jnp.int32)
    my_seg = lax.dynamic_slice_in_dim(seg, start, mine, 0)
    allowed = (my_seg[:, None] == seg[None, :]) & (key_index[None, :] <= query_index[:, None])
    scores = jnp.where(allowed[None, None], scores, -1e30)
    top = jnp.max(scores, axis=-1, keepdims=True)
    expo = jnp.exp(scores - top)
    weights = (expo / jnp.sum(expo, axis=-1, keepdims=True)).astype(jnp.bfloat16)
    context = jnp.einsum("hgqk,khd->qhgd", weights, vals, preferred_element_type=jnp.float32)
    context = context.astype(jnp.bfloat16).reshape(mine, groups * share * HD)
    inner = lax.all_gather(policy_key, "rep", axis=0, tiled=True)
    outer = lax.all_gather(inner, "fsdp", axis=0, tiled=True)
    blocks = policy_key.shape[0]
    shards = outer.shape[0] // (blocks * replicas)
    whole = (
        outer.reshape(shards, replicas, blocks, outer.shape[1])
        .transpose(1, 0, 2, 3)
        .reshape(outer.shape)
    )
    return (context, whole)


def greet(devices, extra, condition):
    barrier = pltpu.get_barrier_semaphore()
    for device in devices:
        pl.semaphore_signal(barrier, inc=1, device_id=device, device_id_type=MESH)

    @pl.when(condition)
    def _():
        pl.semaphore_signal(barrier, inc=1, device_id=extra, device_id_type=MESH)
        pl.semaphore_wait(barrier, len(devices) + 1)

    @pl.when(jnp.logical_not(condition))
    def _():
        pl.semaphore_wait(barrier, len(devices))


class Copies:
    def __init__(self, send, recv, ring):
        self.send, self.recv, self.ring = send, recv, ring
        self.made, self.done, self.left, self.used = [], 0, set(), 0

    def place(self):
        self.used += 1
        return self.used - 1

    def start(self, src, dst, device, sends=None, place=None):
        n = len(self.made)
        self.retire(n - self.ring + 1)
        place = self.place() if place is None else place
        copy = pltpu.make_async_remote_copy(
            src_ref=src, dst_ref=dst, send_sem=self.send.at[n % self.ring], recv_sem=self.recv.at[place],
            device_id=device, device_id_type=MESH,
        )
        only(sends, copy.start)
        self.made.append((copy, sends))
        return copy

    def arrival(self, ref, device, place):
        return pltpu.make_async_remote_copy(
            src_ref=ref, dst_ref=ref, send_sem=self.send.at[0], recv_sem=self.recv.at[place],
            device_id=device, device_id_type=MESH,
        )

    def sent(self, n):
        if n not in self.left:
            self.left.add(n)
            copy, sends = self.made[n]
            only(sends, copy.wait_send)

    def retire(self, count):
        while self.done < count:
            self.sent(self.done)
            self.done += 1


def only(condition, act):
    if condition is None:
        act()
    else:
        pl.when(condition)(act)


def sizes_of(g, groups, share):
    if g == groups - 1:
        return [2] * (share // 2) + [1] * (share % 2)
    return [share - share // 2, share // 2]


def plan(groups, share):
    width = (share + 2) * HD
    pieces = []
    for g in range(groups):
        pair = [("k", g, share), ("v", g, share + 1)]
        pieces += [pair[:1], pair[1:]] if g == 0 else [pair]
    for g in range(groups):
        at = 0
        for size in sizes_of(g, groups, share):
            pieces.append([("q", g, j) for j in range(at, at + size)])
            at += size
    return [(heads[0][1] * width + heads[0][2] * HD, heads) for heads in pieces]


def layer_kernel(
    tok, w, bias, seg, pol, out, pg,
    x, wg, own, fin, snd, inb, kv, shut, cosine, sine, ctx, pv,
    send, recv, w_local, local, z_send, z_recv,
):
    f, r, t = lax.axis_index("fsdp"), lax.axis_index("rep"), lax.axis_index("tp")
    mine = x.shape[0] // 4
    block, columns = w.shape
    hb = block // 2
    share = QH // KVH
    width = (share + 2) * HD
    groups = columns // width
    fx = f + 1 - 2 * lax.rem(f, 2)
    fy = lax.rem(f + 2, 4)
    near = r + 1 - 2 * lax.rem(r, 2)
    across = 3 - r
    end = (r == 0) | (r == 3)
    mid = (r == 1) | (r == 2)
    to_x, to_y, to_near, to_across = {"fsdp": fx}, {"fsdp": fy}, {"rep": near}, {"rep": across}
    to_up, to_down = {"rep": lax.rem(r + 1, 4)}, {"rep": lax.rem(r + 3, 4)}
    copies = Copies(send, recv, RING)

    chunks = plan(groups, share)
    n = len(chunks)
    wide = [len(heads) * HD for _, heads in chunks]
    col = [pl.ds(at, wide[c]) for c, (at, _) in enumerate(chunks)]

    my_rows = pl.ds(pl.multiple_of(f * block, 16), block)
    parts = col[:2] + [pl.ds(width, columns - width), pl.ds(0, share * HD)]
    load_w = [pltpu.make_async_copy(w.at[:, at], wg.at[my_rows, at], w_local.at[i]) for i, at in enumerate(parts)]
    for copy in load_w:
        copy.start()
    loaded = set()
    load_x = pltpu.make_async_copy(tok, x, local.at[0])
    load_p = pltpu.make_async_copy(pol, pv, local.at[1])
    load_p.start()
    load_x.start()
    greet([to_x, to_y, to_near], to_across, mid)

    def held(owner, first, count, c):
        return wg.at[pl.ds(pl.multiple_of(owner * block + first, 16), count), col[c]]

    passed, onwards, last_direct, last_onward = {}, {}, {}, {}

    def direct(c):
        part = c if c < 2 else (3 if chunks[c][0] < width else 2)
        if part not in loaded:
            loaded.add(part)
            load_w[part].wait()
        src = held(f, 0, block, c)
        place = copies.place()
        last_direct[c] = len(copies.made)
        copies.start(src, src, to_x, place=place)
        copies.start(src, src, to_y, place=place)
        passed[c] = copies.arrival(wg.at[pl.ds(0, 2 * block), col[c]], to_x, place)

    def left(c):
        copies.sent(c)
        copies.sent(c + 1)

    def onward(c):
        passed[c].wait_recv()
        place = copies.place()
        copies.start(held(fx, 0, hb, c), held(fx, 0, hb, c), to_y, place=place)
        copies.start(held(fy, hb, hb, c), held(fy, hb, hb, c), to_x, place=place)
        last_onward[c] = len(copies.made) - 2
        onwards[c] = copies.arrival(wg.at[pl.ds(0, block), col[c]], to_x, place)

    def policy_at(j, owner, first=0, count=block):
        return pg.at[pl.ds(pl.multiple_of((j * 4 + owner) * block + first, 16), count)]

    p_up, p_down = {}, {}

    def policy_z(k):
        up_block, down_block = lax.rem(r + 5 - k, 4), lax.rem(r + k - 1, 4)
        up_src = pv if k == 1 else policy_at(up_block, f)
        down_src = pv if k == 1 else policy_at(down_block, f)
        if k > 1:
            landed_z(k - 1)
        p_up[k] = copies.start(up_src, policy_at(up_block, f), to_up, (r <= 2) & (r >= k - 1))
        p_down[k] = copies.start(down_src, policy_at(down_block, f), to_down, (r >= 1) & (r <= 4 - k))

    def landed_z(k):
        only(r >= k, p_up[k].wait_recv)
        only(r <= 3 - k, p_down[k].wait_recv)

    p_direct, p_onward = {}, {}

    def policy_direct(j):
        src, place = policy_at(j, f), copies.place()
        copies.start(src, src, to_x, place=place)
        copies.start(src, src, to_y, place=place)
        p_direct[j] = copies.arrival(pg.at[pl.ds(0, 2 * block)], to_x, place)

    def policy_onward(j):
        p_direct[j].wait_recv()
        place = copies.place()
        copies.start(policy_at(j, fx, 0, hb), policy_at(j, fx, 0, hb), to_y, place=place)
        copies.start(policy_at(j, fy, hb, hb), policy_at(j, fy, hb, hb), to_x, place=place)
        p_onward[j] = copies.arrival(pg.at[pl.ds(0, block)], to_x, place)

    def rows_of(slot):
        ahead = jnp.where(
            slot == 0, 3, jnp.where(slot == 1, 2, jnp.where((slot == 2) == end, 1, 0))
        )
        return jnp.where(r >= 2, 3 - ahead, ahead)

    def product(c, slot):
        rows = pl.ds(pl.multiple_of(rows_of(slot) * mine, mine), mine)
        return jnp.dot(x[rows, :], wg[:, col[c]], preferred_element_type=jnp.float32)

    def hop(c, slot, place, device):
        return pltpu.make_async_remote_copy(
            src_ref=snd.at[slot, :, col[c]], dst_ref=inb.at[place, :, col[c]],
            send_sem=z_send.at[slot, c % HOPS], recv_sem=z_recv.at[z_place(place), c],
            device_id=device, device_id_type=MESH,
        )

    def z_place(place):
        return (0, 1, 3, 2, 3)[place]

    def came(c, place):
        hop(c, 0, place, to_near).wait_recv()

    def came_last(c):
        both = inb.at[pl.ds(0, 2), :, col[c]]
        pair = pltpu.make_async_remote_copy(
            src_ref=both, dst_ref=both, send_sem=z_send.at[0, 0], recv_sem=z_recv.at[3, c],
            device_id=to_near, device_id_type=MESH,
        )
        pl.when(mid)(pair.wait_recv)
        pl.when(end)(hop(c, 0, 2, to_near).wait_recv)

    def work_end(c):
        def one(slot, _):
            snd[slot, :, col[c]] = product(c, slot).astype(jnp.bfloat16)
            pltpu.make_async_remote_copy(
                src_ref=snd.at[slot, :, col[c]], dst_ref=inb.at[slot, :, col[c]],
                send_sem=z_send.at[slot, c % HOPS], recv_sem=z_recv.at[jnp.where(slot == 2, 3, slot), c],
                device_id=to_near, device_id_type=MESH,
            ).start()
            return 0

        lax.fori_loop(0, 3, one, 0)
        fin[:, col[c]] = product(c, 3)

    def work_mid(c):
        here = pl.ds(0, wide[c])

        def one(slot, _):
            own[slot_of(c), slot, :, here] = product(c, slot)
            return 0

        lax.fori_loop(0, 3, one, 0)
        fin[:, col[c]] = product(c, 3)

    def work_one(c):
        if 1 <= c <= n - 3:
            work_back(c - 1)
        if c > n - 3:
            work_back(c)
        if c == n - 1:
            finish(n - 4)
        work_across(c)
        if c == n - 3:
            work_back(c)

    def work_two(c):
        work_across(c)
        if c >= 1:
            work_back(c - 1)

    def work_across(c):
        relay(c, 0, 0, 3, to_across)
        relay(c, 1, 1, 4, to_across)

    def relay(c, slot, source, place, device):
        came(c, source)
        total = own[slot_of(c), slot, :, pl.ds(0, wide[c])] + inb[source, :, col[c]].astype(jnp.float32)
        snd[slot, :, col[c]] = total.astype(jnp.bfloat16)
        hop(c, slot, place, device).start()

    def work_back(c):
        relay(c, 2, 3, 2, to_near)

    def slot_of(c):
        return c % 2

    def summed(at):
        return (
            fin[:, at] + inb[2, :, at].astype(jnp.float32)
            + inb[4, :, at].astype(jnp.float32) + bias[at][None, :]
        )

    def rotated(values):
        return values * cosine[...] + pltpu.roll(values, HD // 2, 1) * sine[...]

    kv_up, kv_on = {}, {}

    def stored(kind, g):
        return pl.ds((2 * g + (kind == "v")) * HD, HD)

    def span(c):
        _, heads = chunks[c]
        return pl.ds((2 * heads[0][1] + (heads[0][0] == "v")) * HD, wide[c])

    key_chunks = [c for c in range(n) if chunks[c][1][0][0] != "q"]
    low, middle, high = (pl.ds(k * mine, mine) for k in range(3))

    def finish_keys(c):
        at, heads = chunks[c]
        for kind, g, j in heads:
            values = summed(pl.ds(at + (j - heads[0][2]) * HD, HD))
            kv[high, stored(kind, g)] = (rotated(values) if kind == "k" else values).astype(jnp.bfloat16)
        kv_up[c] = copies.start(kv.at[high, span(c)], kv.at[middle, span(c)], to_up, r <= 2)

    def forward_keys(c):
        only(r >= 1, kv_up[c].wait_recv)
        kv_on[c] = copies.start(kv.at[middle, span(c)], kv.at[low, span(c)], to_up, mid)

    scale = 1.0 / math.sqrt(HD)
    keys_in = set()

    def attend(c):
        at, heads = chunks[c]
        _, g, first = heads[0]
        for k in key_chunks:
            if k not in keys_in and chunks[k][1][0][1] == g:
                keys_in.add(k)
                only(r >= 2, kv_on[k].wait_recv)
        kc, vc = stored("k", g), stored("v", g)
        base = (g * share + first) * HD

        def head(j, _):
            query = rotated(summed(pl.ds(pl.multiple_of(at + j * HD, HD), HD))).astype(jnp.bfloat16)
            scores = lax.dot_general(
                query, kv[:, kc], (((1,), (1,)), ((), ())), preferred_element_type=jnp.float32
            ) * scale + shut[...]
            expo = jnp.exp(scores - jnp.max(scores, axis=-1, keepdims=True))
            total = jnp.sum(expo, axis=-1, keepdims=True)
            weights = (expo * (1.0 / total)).astype(jnp.bfloat16)
            to = pl.ds(pl.multiple_of(base + j * HD, HD), HD)
            ctx[:, to] = jnp.dot(weights, kv[:, vc], preferred_element_type=jnp.float32).astype(jnp.bfloat16)
            return 0

        lax.fori_loop(0, len(heads), head, 0)
        part = pl.ds(base, wide[c])
        pltpu.make_async_copy(ctx.at[:, part], out.at[:, part], local.at[3]).start()

    def finish(c):
        came_last(c)
        (attend if chunks[c][1][0][0] == "q" else finish_keys)(c)

    def prepare():
        at = pl.ds(pl.multiple_of(r * mine, mine), mine)
        square = (mine, mine)
        row, lane = lax.broadcasted_iota(jnp.int32, square, 0), lax.broadcasted_iota(jnp.int32, square, 1)
        mine_row = jnp.broadcast_to(seg[:, at].astype(jnp.float32), square)
        my_seg = jnp.sum(jnp.where(row == lane, mine_row, 0.0), axis=-1, keepdims=True)
        before = jnp.where(seg[...].astype(jnp.float32) < my_seg, 1.0, 0.0)
        first = jnp.sum(before, axis=-1, keepdims=True)
        index = lax.broadcasted_iota(jnp.int32, (mine, HD), 0) + r * mine
        half = HD // 2
        place = lax.rem(lax.broadcasted_iota(jnp.int32, (1, HD), 1), half)
        freq = jnp.ones((1, HD), jnp.float32)
        for i in range(1, half):
            freq = jnp.where(place == i, 1000000.0 ** (-2.0 * i / HD), freq)
        angle = (index.astype(jnp.float32) - first) * freq
        cosine[...] = jnp.cos(angle)
        wave = jnp.sin(angle)
        sine[...] = jnp.where(lax.broadcasted_iota(jnp.int32, (mine, HD), 1) < half, -wave, wave)
        for slot in range(3):
            there = r - 2 + slot
            keys = pl.ds(pl.multiple_of(jnp.maximum(there, 0) * mine, mine), mine)
            allowed = (my_seg == seg[:, keys].astype(jnp.float32)) & (there >= 0)
            if slot == 2:
                allowed = allowed & (lane <= row)
            shut[:, slot * mine:(slot + 1) * mine] = jnp.where(allowed, 0.0, -1e30)

        @pl.when(r <= 1)
        def _():
            kv[low, :] = jnp.zeros((mine, kv.shape[1]), kv.dtype)

        @pl.when(r == 0)
        def _():
            kv[middle, :] = jnp.zeros((mine, kv.shape[1]), kv.dtype)

        @pl.when(end)
        def _():
            inb[4] = jnp.zeros(inb.shape[1:], inb.dtype)

    def weights_in(c):
        onwards[c].wait_recv()

    queries = len(key_chunks)
    direct(0)
    load_p.wait()
    policy_z(1)
    keep_p = pltpu.make_async_copy(pv, policy_at(r, f), local.at[2])
    keep_p.start()
    left(last_direct[0])
    direct(1)
    onward(0)
    left(last_onward[0])
    direct(2)
    onward(1)
    left(last_onward[1])
    direct(3)
    load_x.wait()
    weights_in(0)
    pl.when(end)(functools.partial(work_end, 0))
    onward(2)
    direct(4)
    prepare()
    policy_steps = {
        queries - 1: [("d", 0)], queries: [("d", 1)], queries + 1: [("o", 0), ("d", 2)], queries + 2: [("o", 1)],
        queries + 3: [("d", 3), ("o", 2)], queries + 5: [("o", 3)],
    }

    def weights_on(c):
        if c + 3 < n:
            onward(c + 3)
        if c + 5 < n:
            direct(c + 5)

    def sends_out(c):
        for slot in range(3):
            hop(c, slot, 0, to_near).wait_send()

    for c in range(n):
        if c + 1 >= HOPS:
            sends_out(c + 1 - HOPS)
        if 0 <= c - 4 < queries:
            forward_keys(c - 4)
        early = c - 2 < queries - 2
        if 0 <= c - 2 < queries and not early:
            finish(c - 2)
        if c + 1 < n:
            weights_in(c + 1)
            pl.when(end)(functools.partial(work_end, c + 1))
        if 0 <= c - 2 and early:
            finish(c - 2)
        if c < 3:
            weights_on(c)
        if c == 0:
            policy_z(2)
        if c == 2:
            policy_z(3)
        pl.when(mid)(functools.partial(work_mid, c))
        pl.when(r == 1)(functools.partial(work_one, c))
        pl.when(r == 2)(functools.partial(work_two, c))
        if c >= 3:
            weights_on(c)
        if c == queries - 1:
            landed_z(3)
            keep_p.wait()
        for kind, j in policy_steps.get(c, ()):
            (policy_direct if kind == "d" else policy_onward)(j)
        if queries <= c - 2 < n - 4:
            finish(c - 2)
        if c == n - 2:
            pl.when(r != 1)(functools.partial(finish, n - 4))
    finish(n - 3)
    finish(n - 2)
    pl.when(r == 2)(functools.partial(work_back, n - 1))
    finish(n - 1)
    for j in range(4):
        p_onward[j].wait_recv()
    for c in range(n + 1 - HOPS, n):
        sends_out(c)
    copies.retire(len(copies.made))
    pltpu.make_async_copy(ctx, out, local.at[3]).wait()


def settle_kernel(ctx, pg, out, whole, store):
    step = pg.shape[0] // PIECES
    stores = [(pg.at[pl.ds(k * step, step)], whole.at[pl.ds(k * step, step)]) for k in range(PIECES)] + [(ctx, out)]
    stores = [pltpu.make_async_copy(src, dst, store.at[i]) for i, (src, dst) in enumerate(stores)]
    for copy in stores:
        copy.start()
    for copy in stores:
        copy.wait()


def whole_layer(tokens, ref_qkv, ref_bias, segment_ids, policy_key):
    rows, depth = tokens.shape
    block, columns = ref_qkv.shape
    mine, share = rows // 4, QH // KVH
    groups = columns // ((share + 2) * HD)
    chunks = plan(groups, share)
    n = len(chunks)
    keys = sum(heads[0][0] != "q" for _, heads in chunks)
    widest = max(len(heads) for _, heads in chunks) * HD
    places = 2 * n + 6 + 2 * keys + 8
    hbm, vmem = pl.BlockSpec(memory_space=pltpu.HBM), pl.BlockSpec(memory_space=pltpu.VMEM)
    any_space = pl.BlockSpec(memory_space=pl.ANY)
    low, full = jnp.bfloat16, jnp.float32
    dma = pltpu.SemaphoreType.DMA
    out, pg = pl.pallas_call(
        layer_kernel,
        out_shape=(
            pltpu.VMEM((mine, groups * share * HD), low),
            pltpu.VMEM((16 * block, policy_key.shape[1]), policy_key.dtype),
        ),
        in_specs=[hbm, hbm, vmem, vmem, hbm],
        out_specs=(any_space, any_space),
        scratch_shapes=[
            pltpu.VMEM((rows, depth), tokens.dtype),
            pltpu.VMEM((4 * block, columns), ref_qkv.dtype),
            pltpu.VMEM((2, 3, mine, widest), full),
            pltpu.VMEM((mine, columns), full),
            pltpu.VMEM((3, mine, columns), low),
            pltpu.VMEM((5, mine, columns), low),
            pltpu.VMEM((3 * mine, groups * 2 * HD), low),
            pltpu.VMEM((mine, 3 * mine), full),
            pltpu.VMEM((mine, HD), full),
            pltpu.VMEM((mine, HD), full),
            pltpu.VMEM((mine, groups * share * HD), low),
            pltpu.VMEM(policy_key.shape, policy_key.dtype),
            dma((RING,)),
            dma((places,)),
            dma((4,)),
            dma((4,)),
            dma((3, HOPS)),
            dma((4, n)),
        ],
        compiler_params=pltpu.CompilerParams(
            collective_id=0, has_side_effects=True, vmem_limit_bytes=VMEM_LIMIT
        ),
    )(tokens, ref_qkv, ref_bias, segment_ids, policy_key)
    return pl.pallas_call(
        settle_kernel,
        out_shape=tuple(jax.ShapeDtypeStruct(a.shape, a.dtype) for a in (out, pg)),
        in_specs=[any_space] * 2,
        out_specs=(any_space,) * 2,
        scratch_shapes=[dma((PIECES + 1,))],
        compiler_params=pltpu.CompilerParams(vmem_limit_bytes=VMEM_LIMIT),
    )(*(pltpu.with_memory_space_constraint(a, pltpu.VMEM) for a in (out, pg)))


PIECES = 4
VMEM_LIMIT = 50 * 1024 * 1024
RING = 32
HOPS = 4


def solution(mesh):
    in_specs = (
        P("fsdp", "rep"),
        P(("rep", "fsdp"), "tp"),
        P("tp"),
        P("fsdp", None),
        P(("rep", "fsdp"), "tp"),
    )
    out_specs = (P(("fsdp", "rep"), "tp"), P(None, "tp"))
    shape = mesh.shape
    grouped = shape["rep"] == 4 and shape["fsdp"] == 4 and shape["tp"] == 2
    return jax.shard_map(
        whole_layer if grouped else per_device, mesh=mesh, in_specs=in_specs, out_specs=out_specs, check_vma=False
    )
```

```python
import jax
import jax.numpy as jnp
from jax import lax
from jax.experimental import pallas as pl
from jax.experimental.pallas import tpu as pltpu
from jax.sharding import PartitionSpec as P
import functools
import math

MESH = pl.DeviceIdType.MESH

QH = 40
KVH = 8
HD = 128


def positions_of(seg):
    count = seg.shape[0]
    index = jnp.arange(count, dtype=jnp.int32)
    starts = jnp.concatenate([jnp.ones((1,), bool), seg[1:] != seg[:-1]])
    first = lax.cummax(jnp.where(starts, index, 0), axis=0)
    return index - first


def rotary(values, pos):
    half = values.shape[-1] // 2
    freq = 1000000.0 ** (-2.0 * jnp.arange(half, dtype=jnp.float32) / values.shape[-1])
    angle = pos.astype(jnp.float32)[:, None] * freq[None, :]
    shape = (values.shape[0],) + (1,) * (values.ndim - 2) + (half,)
    cosine = jnp.cos(angle).reshape(shape)
    sine = jnp.sin(angle).reshape(shape)
    first = values[..., :half]
    second = values[..., half:]
    return jnp.concatenate(
        [first * cosine - second * sine, second * cosine + first * sine], axis=-1
    )


def per_device(tokens, ref_qkv, ref_bias, segment_ids, policy_key):
    share = QH // KVH
    rows = tokens.shape[0]
    columns = ref_qkv.shape[1]
    groups = columns // ((share + 2) * HD)
    replicas = lax.axis_size("rep")
    mine = rows // replicas
    rank = lax.axis_index("rep")
    partial_value = jnp.dot(
        tokens,
        lax.all_gather(ref_qkv, "fsdp", axis=0, tiled=True),
        preferred_element_type=jnp.float32,
    )
    partial_value = partial_value.reshape(rows, groups, share + 2, HD)
    bias = ref_bias.reshape(groups, share + 2, HD)
    seg = segment_ids[0]
    pos = positions_of(seg)
    start = rank * mine
    my_pos = lax.dynamic_slice_in_dim(pos, start, mine, 0)
    summed = lax.psum_scatter(partial_value, "rep", scatter_dimension=0, tiled=True) + bias[None]
    query = rotary(summed[:, :, :share], my_pos).astype(jnp.bfloat16)
    my_keys = rotary(summed[:, :, share], my_pos).astype(jnp.bfloat16)
    my_vals = summed[:, :, share + 1].astype(jnp.bfloat16)
    keys, vals = (
        lax.all_gather(my_keys, "rep", axis=0, tiled=True),
        lax.all_gather(my_vals, "rep", axis=0, tiled=True),
    )
    scores = jnp.einsum(
        "qhgd,khd->hgqk", query, keys, preferred_element_type=jnp.float32
    ) / jnp.sqrt(jnp.float32(HD))
    query_index = start + jnp.arange(mine, dtype=jnp.int32)
    key_index = jnp.arange(rows, dtype=jnp.int32)
    my_seg = lax.dynamic_slice_in_dim(seg, start, mine, 0)
    allowed = (my_seg[:, None] == seg[None, :]) & (key_index[None, :] <= query_index[:, None])
    scores = jnp.where(allowed[None, None], scores, -1e30)
    top = jnp.max(scores, axis=-1, keepdims=True)
    expo = jnp.exp(scores - top)
    weights = (expo / jnp.sum(expo, axis=-1, keepdims=True)).astype(jnp.bfloat16)
    context = jnp.einsum("hgqk,khd->qhgd", weights, vals, preferred_element_type=jnp.float32)
    context = context.astype(jnp.bfloat16).reshape(mine, groups * share * HD)
    inner = lax.all_gather(policy_key, "rep", axis=0, tiled=True)
    outer = lax.all_gather(inner, "fsdp", axis=0, tiled=True)
    blocks = policy_key.shape[0]
    shards = outer.shape[0] // (blocks * replicas)
    whole = (
        outer.reshape(shards, replicas, blocks, outer.shape[1])
        .transpose(1, 0, 2, 3)
        .reshape(outer.shape)
    )
    return (context, whole)


def greet(devices, extra, condition):
    barrier = pltpu.get_barrier_semaphore()
    for device in devices:
        pl.semaphore_signal(barrier, inc=1, device_id=device, device_id_type=MESH)

    @pl.when(condition)
    def _():
        pl.semaphore_signal(barrier, inc=1, device_id=extra, device_id_type=MESH)
        pl.semaphore_wait(barrier, len(devices) + 1)

    @pl.when(jnp.logical_not(condition))
    def _():
        pl.semaphore_wait(barrier, len(devices))


class Copies:
    def __init__(self, send, recv, ring):
        self.send, self.recv, self.ring = send, recv, ring
        self.made, self.done, self.left, self.used = [], 0, set(), 0

    def place(self):
        self.used += 1
        return self.used - 1

    def start(self, src, dst, device, sends=None, place=None):
        n = len(self.made)
        self.retire(n - self.ring + 1)
        place = self.place() if place is None else place
        copy = pltpu.make_async_remote_copy(
            src_ref=src, dst_ref=dst, send_sem=self.send.at[n % self.ring], recv_sem=self.recv.at[place],
            device_id=device, device_id_type=MESH,
        )
        only(sends, copy.start)
        self.made.append((copy, sends))
        return copy

    def arrival(self, ref, device, place):
        return pltpu.make_async_remote_copy(
            src_ref=ref, dst_ref=ref, send_sem=self.send.at[0], recv_sem=self.recv.at[place],
            device_id=device, device_id_type=MESH,
        )

    def sent(self, n):
        if n not in self.left:
            self.left.add(n)
            copy, sends = self.made[n]
            only(sends, copy.wait_send)

    def retire(self, count):
        while self.done < count:
            self.sent(self.done)
            self.done += 1


def only(condition, act):
    if condition is None:
        act()
    else:
        pl.when(condition)(act)


def sizes_of(g, groups, share):
    if g == groups - 1:
        return [2] * (share // 2) + [1] * (share % 2)
    return [share - share // 2, share // 2]


def plan(groups, share):
    width = (share + 2) * HD
    pieces = []
    for g in range(groups):
        pair = [("k", g, share), ("v", g, share + 1)]
        pieces += [pair[:1], pair[1:]] if g == 0 else [pair]
    for g in range(groups):
        at = 0
        for size in sizes_of(g, groups, share):
            pieces.append([("q", g, j) for j in range(at, at + size)])
            at += size
    return [(heads[0][1] * width + heads[0][2] * HD, heads) for heads in pieces]


def layer_kernel(
    tok, w, bias, seg, pol, out, pg,
    x, wg, own, fin, snd, inb, kv, shut, cosine, sine, ctx, pv,
    send, recv, w_local, local, z_send, z_recv,
):
    f, r, t = lax.axis_index("fsdp"), lax.axis_index("rep"), lax.axis_index("tp")
    mine = x.shape[0] // 4
    block, columns = w.shape
    hb = block // 2
    share = QH // KVH
    width = (share + 2) * HD
    groups = columns // width
    fx = f + 1 - 2 * lax.rem(f, 2)
    fy = lax.rem(f + 2, 4)
    near = r + 1 - 2 * lax.rem(r, 2)
    across = 3 - r
    end = (r == 0) | (r == 3)
    mid = (r == 1) | (r == 2)
    to_x, to_y, to_near, to_across = {"fsdp": fx}, {"fsdp": fy}, {"rep": near}, {"rep": across}
    to_up, to_down = {"rep": lax.rem(r + 1, 4)}, {"rep": lax.rem(r + 3, 4)}
    copies = Copies(send, recv, RING)

    chunks = plan(groups, share)
    n = len(chunks)
    wide = [len(heads) * HD for _, heads in chunks]
    col = [pl.ds(at, wide[c]) for c, (at, _) in enumerate(chunks)]

    my_rows = pl.ds(pl.multiple_of(f * block, 16), block)
    parts = col[:2] + [pl.ds(width, columns - width), pl.ds(0, share * HD)]
    load_w = [pltpu.make_async_copy(w.at[:, at], wg.at[my_rows, at], w_local.at[i]) for i, at in enumerate(parts)]
    for copy in load_w:
        copy.start()
    loaded = set()
    load_x = pltpu.make_async_copy(tok, x, local.at[0])
    load_p = pltpu.make_async_copy(pol, pv, local.at[1])
    load_p.start()
    load_x.start()
    greet([to_x, to_y, to_near], to_across, mid)

    def held(owner, first, count, c):
        return wg.at[pl.ds(pl.multiple_of(owner * block + first, 16), count), col[c]]

    passed, onwards, last_direct, last_onward = {}, {}, {}, {}

    def direct(c):
        part = c if c < 2 else (3 if chunks[c][0] < width else 2)
        if part not in loaded:
            loaded.add(part)
            load_w[part].wait()
        src = held(f, 0, block, c)
        place = copies.place()
        last_direct[c] = len(copies.made)
        copies.start(src, src, to_x, place=place)
        copies.start(src, src, to_y, place=place)
        passed[c] = copies.arrival(wg.at[pl.ds(0, 2 * block), col[c]], to_x, place)

    def left(c):
        copies.sent(c)
        copies.sent(c + 1)

    def onward(c):
        passed[c].wait_recv()
        place = copies.place()
        copies.start(held(fx, 0, hb, c), held(fx, 0, hb, c), to_y, place=place)
        copies.start(held(fy, hb, hb, c), held(fy, hb, hb, c), to_x, place=place)
        last_onward[c] = len(copies.made) - 2
        onwards[c] = copies.arrival(wg.at[pl.ds(0, block), col[c]], to_x, place)

    def policy_at(j, owner, first=0, count=block):
        return pg.at[pl.ds(pl.multiple_of((j * 4 + owner) * block + first, 16), count)]

    p_up, p_down = {}, {}

    def policy_z(k):
        up_block, down_block = lax.rem(r + 5 - k, 4), lax.rem(r + k - 1, 4)
        up_src = pv if k == 1 else policy_at(up_block, f)
        down_src = pv if k == 1 else policy_at(down_block, f)
        if k > 1:
            landed_z(k - 1)
        p_up[k] = copies.start(up_src, policy_at(up_block, f), to_up, (r <= 2) & (r >= k - 1))
        p_down[k] = copies.start(down_src, policy_at(down_block, f), to_down, (r >= 1) & (r <= 4 - k))

    def landed_z(k):
        only(r >= k, p_up[k].wait_recv)
        only(r <= 3 - k, p_down[k].wait_recv)

    p_direct, p_onward = {}, {}

    def policy_direct(j):
        src, place = policy_at(j, f), copies.place()
        copies.start(src, src, to_x, place=place)
        copies.start(src, src, to_y, place=place)
        p_direct[j] = copies.arrival(pg.at[pl.ds(0, 2 * block)], to_x, place)

    def policy_onward(j):
        p_direct[j].wait_recv()
        place = copies.place()
        copies.start(policy_at(j, fx, 0, hb), policy_at(j, fx, 0, hb), to_y, place=place)
        copies.start(policy_at(j, fy, hb, hb), policy_at(j, fy, hb, hb), to_x, place=place)
        p_onward[j] = copies.arrival(pg.at[pl.ds(0, block)], to_x, place)

    def rows_of(slot):
        ahead = jnp.where(
            slot == 0, 3, jnp.where(slot == 1, 2, jnp.where((slot == 2) == end, 1, 0))
        )
        return jnp.where(r >= 2, 3 - ahead, ahead)

    def product(c, slot):
        rows = pl.ds(pl.multiple_of(rows_of(slot) * mine, mine), mine)
        return jnp.dot(x[rows, :], wg[:, col[c]], preferred_element_type=jnp.float32)

    def hop(c, slot, place, device):
        return pltpu.make_async_remote_copy(
            src_ref=snd.at[slot, :, col[c]], dst_ref=inb.at[place, :, col[c]],
            send_sem=z_send.at[slot, c % HOPS], recv_sem=z_recv.at[z_place(place), c],
            device_id=device, device_id_type=MESH,
        )

    def z_place(place):
        return (0, 1, 3, 2, 3)[place]

    def came(c, place):
        hop(c, 0, place, to_near).wait_recv()

    def came_last(c):
        both = inb.at[pl.ds(0, 2), :, col[c]]
        pair = pltpu.make_async_remote_copy(
            src_ref=both, dst_ref=both, send_sem=z_send.at[0, 0], recv_sem=z_recv.at[3, c],
            device_id=to_near, device_id_type=MESH,
        )
        pl.when(mid)(pair.wait_recv)
        pl.when(end)(hop(c, 0, 2, to_near).wait_recv)

    def work_end(*several):
        def one(slot, _):
            for c in several:
                snd[slot, :, col[c]] = product(c, slot).astype(jnp.bfloat16)
                pltpu.make_async_remote_copy(
                    src_ref=snd.at[slot, :, col[c]], dst_ref=inb.at[slot, :, col[c]],
                    send_sem=z_send.at[slot, c % HOPS], recv_sem=z_recv.at[jnp.where(slot == 2, 3, slot), c],
                    device_id=to_near, device_id_type=MESH,
                ).start()
            return 0

        lax.fori_loop(0, 3, one, 0)
        for c in several:
            fin[:, col[c]] = product(c, 3)

    def work_mid(c):
        here = pl.ds(0, wide[c])

        def one(slot, _):
            own[slot_of(c), slot, :, here] = product(c, slot)
            return 0

        lax.fori_loop(0, 3, one, 0)
        fin[:, col[c]] = product(c, 3)

    def work_one(c):
        if c >= 1:
            work_back(c - 1)
        work_across(c)
        if c == n - 3:
            work_back(c)

    def work_two(c):
        work_across(c)
        if c >= 1:
            work_back(c - 1)

    def work_across(*several):
        for slot in range(2):
            for c in several:
                relay(c, slot, slot, 3 + slot, to_across)

    def last_one():
        work_back(n - 2)
        work_back(n - 1)
        work_across(n - 2, n - 1)

    def last_two():
        work_across(n - 2, n - 1)
        work_back(n - 3)

    def last_back():
        work_back(n - 2)
        work_back(n - 1)

    def relay(c, slot, source, place, device):
        came(c, source)
        total = own[slot_of(c), slot, :, pl.ds(0, wide[c])] + inb[source, :, col[c]].astype(jnp.float32)
        snd[slot, :, col[c]] = total.astype(jnp.bfloat16)
        hop(c, slot, place, device).start()

    def work_back(c):
        relay(c, 2, 3, 2, to_near)

    def slot_of(c):
        return c % 3

    def summed(at):
        return (
            fin[:, at] + inb[2, :, at].astype(jnp.float32)
            + inb[4, :, at].astype(jnp.float32) + bias[at][None, :]
        )

    def rotated(values):
        return values * cosine[...] + pltpu.roll(values, HD // 2, 1) * sine[...]

    kv_up, kv_on = {}, {}

    def stored(kind, g):
        return pl.ds((2 * g + (kind == "v")) * HD, HD)

    def span(c):
        _, heads = chunks[c]
        return pl.ds((2 * heads[0][1] + (heads[0][0] == "v")) * HD, wide[c])

    key_chunks = [c for c in range(n) if chunks[c][1][0][0] != "q"]
    low, middle, high = (pl.ds(k * mine, mine) for k in range(3))

    def finish_keys(c):
        at, heads = chunks[c]
        for kind, g, j in heads:
            values = summed(pl.ds(at + (j - heads[0][2]) * HD, HD))
            kv[high, stored(kind, g)] = (rotated(values) if kind == "k" else values).astype(jnp.bfloat16)
        kv_up[c] = copies.start(kv.at[high, span(c)], kv.at[middle, span(c)], to_up, r <= 2)

    def forward_keys(c):
        only(r >= 1, kv_up[c].wait_recv)
        kv_on[c] = copies.start(kv.at[middle, span(c)], kv.at[low, span(c)], to_up, mid)

    scale = 1.0 / math.sqrt(HD)
    keys_in = set()

    def attend(c):
        at, heads = chunks[c]
        _, g, first = heads[0]
        for k in key_chunks:
            if k not in keys_in and chunks[k][1][0][1] == g:
                keys_in.add(k)
                only(r >= 2, kv_on[k].wait_recv)
        kc, vc = stored("k", g), stored("v", g)
        base = (g * share + first) * HD

        def head(j, _):
            query = rotated(summed(pl.ds(pl.multiple_of(at + j * HD, HD), HD))).astype(jnp.bfloat16)
            scores = lax.dot_general(
                query, kv[:, kc], (((1,), (1,)), ((), ())), preferred_element_type=jnp.float32
            ) * scale + shut[...]
            expo = jnp.exp(scores - jnp.max(scores, axis=-1, keepdims=True))
            total = jnp.sum(expo, axis=-1, keepdims=True)
            weights = (expo * (1.0 / total)).astype(jnp.bfloat16)
            to = pl.ds(pl.multiple_of(base + j * HD, HD), HD)
            ctx[:, to] = jnp.dot(weights, kv[:, vc], preferred_element_type=jnp.float32).astype(jnp.bfloat16)
            return 0

        lax.fori_loop(0, len(heads), head, 0)
        part = pl.ds(base, wide[c])
        pltpu.make_async_copy(ctx.at[:, part], out.at[:, part], local.at[3]).start()

    def finish(c):
        came_last(c)
        (attend if chunks[c][1][0][0] == "q" else finish_keys)(c)

    def prepare():
        at = pl.ds(pl.multiple_of(r * mine, mine), mine)
        square = (mine, mine)
        row, lane = lax.broadcasted_iota(jnp.int32, square, 0), lax.broadcasted_iota(jnp.int32, square, 1)
        mine_row = jnp.broadcast_to(seg[:, at].astype(jnp.float32), square)
        my_seg = jnp.sum(jnp.where(row == lane, mine_row, 0.0), axis=-1, keepdims=True)
        before = jnp.where(seg[...].astype(jnp.float32) < my_seg, 1.0, 0.0)
        first = jnp.sum(before, axis=-1, keepdims=True)
        index = lax.broadcasted_iota(jnp.int32, (mine, HD), 0) + r * mine
        half = HD // 2
        place = lax.rem(lax.broadcasted_iota(jnp.int32, (1, HD), 1), half)
        freq = jnp.ones((1, HD), jnp.float32)
        for i in range(1, half):
            freq = jnp.where(place == i, 1000000.0 ** (-2.0 * i / HD), freq)
        angle = (index.astype(jnp.float32) - first) * freq
        cosine[...] = jnp.cos(angle)
        wave = jnp.sin(angle)
        sine[...] = jnp.where(lax.broadcasted_iota(jnp.int32, (mine, HD), 1) < half, -wave, wave)
        for slot in range(3):
            there = r - 2 + slot
            keys = pl.ds(pl.multiple_of(jnp.maximum(there, 0) * mine, mine), mine)
            allowed = (my_seg == seg[:, keys].astype(jnp.float32)) & (there >= 0)
            if slot == 2:
                allowed = allowed & (lane <= row)
            shut[:, slot * mine:(slot + 1) * mine] = jnp.where(allowed, 0.0, -1e30)

        @pl.when(r <= 1)
        def _():
            kv[low, :] = jnp.zeros((mine, kv.shape[1]), kv.dtype)

        @pl.when(r == 0)
        def _():
            kv[middle, :] = jnp.zeros((mine, kv.shape[1]), kv.dtype)

        @pl.when(end)
        def _():
            inb[4] = jnp.zeros(inb.shape[1:], inb.dtype)

    def weights_in(c):
        onwards[c].wait_recv()

    queries = len(key_chunks)
    direct(0)
    load_p.wait()
    policy_z(1)
    keep_p = pltpu.make_async_copy(pv, policy_at(r, f), local.at[2])
    keep_p.start()
    left(last_direct[0])
    direct(1)
    onward(0)
    onward(1)
    load_x.wait()
    weights_in(0)
    direct(2)
    pl.when(end)(functools.partial(work_end, 0))
    policy_steps = {
        queries - 1: [("d", 0)], queries: [("d", 1)], queries + 1: [("o", 0), ("d", 2)], queries + 2: [("o", 1)],
        queries + 3: [("d", 3), ("o", 2)], queries + 5: [("o", 3)],
    }

    weight_steps = {0: "o2 d3", 1: "o3 d4", 2: "o4 d5", 3: "o5 d6 d7", 4: "o6 o7 d8 d9"}

    def weights_on(c):
        for word in weight_steps.get(c, f"o{c + 3} d{c + 5}").split():
            if int(word[1:]) < n:
                (direct if word[0] == "d" else onward)(int(word[1:]))

    def sends_out(c):
        for slot in range(3):
            hop(c, slot, 0, to_near).wait_send()

    for c in range(n - 2):
        ahead = [c + 1] if c < n - 3 else [n - 2, n - 1]
        for k in ahead:
            if k >= HOPS:
                sends_out(k - HOPS)
        if 0 <= c - 4 < queries:
            forward_keys(c - 4)
        early = c - 2 < queries - 2
        if 0 <= c - 2 < queries and not early:
            finish(c - 2)
        for k in ahead:
            weights_in(k)
        pl.when(end)(functools.partial(work_end, *ahead))
        if 0 <= c - 2 and early:
            finish(c - 2)
        if c < 3:
            weights_on(c)
        if c == 0:
            prepare()
            policy_z(2)
        if c == 2:
            policy_z(3)
        pl.when(mid)(functools.partial(work_mid, c))
        pl.when(r == 1)(functools.partial(work_one, c))
        pl.when(r == 2)(functools.partial(work_two, c))
        if c >= 3:
            weights_on(c)
        if c == queries - 1:
            landed_z(3)
            keep_p.wait()
        for kind, j in policy_steps.get(c, ()):
            (policy_direct if kind == "d" else policy_onward)(j)
        if queries <= c - 2:
            finish(c - 2)
    for c in (n - 2, n - 1):
        pl.when(mid)(functools.partial(work_mid, c))
    pl.when(r == 1)(last_one)
    pl.when(r == 2)(last_two)
    finish(n - 4)
    finish(n - 3)
    pl.when(r == 2)(last_back)
    finish(n - 2)
    finish(n - 1)
    for j in range(4):
        p_onward[j].wait_recv()
    for c in range(n - HOPS, n):
        sends_out(c)
    copies.retire(len(copies.made))
    pltpu.make_async_copy(ctx, out, local.at[3]).wait()


def settle_kernel(ctx, pg, out, whole, store):
    step = pg.shape[0] // PIECES
    stores = [(pg.at[pl.ds(k * step, step)], whole.at[pl.ds(k * step, step)]) for k in range(PIECES)] + [(ctx, out)]
    stores = [pltpu.make_async_copy(src, dst, store.at[i]) for i, (src, dst) in enumerate(stores)]
    for copy in stores:
        copy.start()
    for copy in stores:
        copy.wait()


def whole_layer(tokens, ref_qkv, ref_bias, segment_ids, policy_key):
    rows, depth = tokens.shape
    block, columns = ref_qkv.shape
    mine, share = rows // 4, QH // KVH
    groups = columns // ((share + 2) * HD)
    chunks = plan(groups, share)
    n = len(chunks)
    keys = sum(heads[0][0] != "q" for _, heads in chunks)
    widest = max(len(heads) for _, heads in chunks) * HD
    places = 2 * n + 6 + 2 * keys + 8
    hbm, vmem = pl.BlockSpec(memory_space=pltpu.HBM), pl.BlockSpec(memory_space=pltpu.VMEM)
    any_space = pl.BlockSpec(memory_space=pl.ANY)
    low, full = jnp.bfloat16, jnp.float32
    dma = pltpu.SemaphoreType.DMA
    out, pg = pl.pallas_call(
        layer_kernel,
        out_shape=(
            pltpu.VMEM((mine, groups * share * HD), low),
            pltpu.VMEM((16 * block, policy_key.shape[1]), policy_key.dtype),
        ),
        in_specs=[hbm, hbm, vmem, vmem, hbm],
        out_specs=(any_space, any_space),
        scratch_shapes=[
            pltpu.VMEM((rows, depth), tokens.dtype),
            pltpu.VMEM((4 * block, columns), ref_qkv.dtype),
            pltpu.VMEM((3, 3, mine, widest), full),
            pltpu.VMEM((mine, columns), full),
            pltpu.VMEM((3, mine, columns), low),
            pltpu.VMEM((5, mine, columns), low),
            pltpu.VMEM((3 * mine, groups * 2 * HD), low),
            pltpu.VMEM((mine, 3 * mine), full),
            pltpu.VMEM((mine, HD), full),
            pltpu.VMEM((mine, HD), full),
            pltpu.VMEM((mine, groups * share * HD), low),
            pltpu.VMEM(policy_key.shape, policy_key.dtype),
            dma((RING,)),
            dma((places,)),
            dma((4,)),
            dma((4,)),
            dma((3, HOPS)),
            dma((4, n)),
        ],
        compiler_params=pltpu.CompilerParams(
            collective_id=0, has_side_effects=True, vmem_limit_bytes=VMEM_LIMIT
        ),
    )(tokens, ref_qkv, ref_bias, segment_ids, policy_key)
    return pl.pallas_call(
        settle_kernel,
        out_shape=tuple(jax.ShapeDtypeStruct(a.shape, a.dtype) for a in (out, pg)),
        in_specs=[any_space] * 2,
        out_specs=(any_space,) * 2,
        scratch_shapes=[dma((PIECES + 1,))],
        compiler_params=pltpu.CompilerParams(vmem_limit_bytes=VMEM_LIMIT),
    )(*(pltpu.with_memory_space_constraint(a, pltpu.VMEM) for a in (out, pg)))


PIECES = 4
VMEM_LIMIT = 50 * 1024 * 1024
RING = 32
HOPS = 4


def solution(mesh):
    in_specs = (
        P("fsdp", "rep"),
        P(("rep", "fsdp"), "tp"),
        P("tp"),
        P("fsdp", None),
        P(("rep", "fsdp"), "tp"),
    )
    out_specs = (P(("fsdp", "rep"), "tp"), P(None, "tp"))
    shape = mesh.shape
    grouped = shape["rep"] == 4 and shape["fsdp"] == 4 and shape["tp"] == 2
    return jax.shard_map(
        whole_layer if grouped else per_device, mesh=mesh, in_specs=in_specs, out_specs=out_specs, check_vma=False
    )
```

```python
import jax
import jax.numpy as jnp
from jax import lax
from jax.experimental import pallas as pl
from jax.experimental.pallas import tpu as pltpu
from jax.sharding import PartitionSpec as P
import functools
import math

MESH = pl.DeviceIdType.MESH

QH = 40
KVH = 8
HD = 128


def positions_of(seg):
    count = seg.shape[0]
    index = jnp.arange(count, dtype=jnp.int32)
    starts = jnp.concatenate([jnp.ones((1,), bool), seg[1:] != seg[:-1]])
    first = lax.cummax(jnp.where(starts, index, 0), axis=0)
    return index - first


def rotary(values, pos):
    half = values.shape[-1] // 2
    freq = 1000000.0 ** (-2.0 * jnp.arange(half, dtype=jnp.float32) / values.shape[-1])
    angle = pos.astype(jnp.float32)[:, None] * freq[None, :]
    shape = (values.shape[0],) + (1,) * (values.ndim - 2) + (half,)
    cosine = jnp.cos(angle).reshape(shape)
    sine = jnp.sin(angle).reshape(shape)
    first = values[..., :half]
    second = values[..., half:]
    return jnp.concatenate(
        [first * cosine - second * sine, second * cosine + first * sine], axis=-1
    )


def per_device(tokens, ref_qkv, ref_bias, segment_ids, policy_key):
    share = QH // KVH
    rows = tokens.shape[0]
    columns = ref_qkv.shape[1]
    groups = columns // ((share + 2) * HD)
    replicas = lax.axis_size("rep")
    mine = rows // replicas
    rank = lax.axis_index("rep")
    partial_value = jnp.dot(
        tokens,
        lax.all_gather(ref_qkv, "fsdp", axis=0, tiled=True),
        preferred_element_type=jnp.float32,
    )
    partial_value = partial_value.reshape(rows, groups, share + 2, HD)
    bias = ref_bias.reshape(groups, share + 2, HD)
    seg = segment_ids[0]
    pos = positions_of(seg)
    start = rank * mine
    my_pos = lax.dynamic_slice_in_dim(pos, start, mine, 0)
    summed = lax.psum_scatter(partial_value, "rep", scatter_dimension=0, tiled=True) + bias[None]
    query = rotary(summed[:, :, :share], my_pos).astype(jnp.bfloat16)
    my_keys = rotary(summed[:, :, share], my_pos).astype(jnp.bfloat16)
    my_vals = summed[:, :, share + 1].astype(jnp.bfloat16)
    keys, vals = (
        lax.all_gather(my_keys, "rep", axis=0, tiled=True),
        lax.all_gather(my_vals, "rep", axis=0, tiled=True),
    )
    scores = jnp.einsum(
        "qhgd,khd->hgqk", query, keys, preferred_element_type=jnp.float32
    ) / jnp.sqrt(jnp.float32(HD))
    query_index = start + jnp.arange(mine, dtype=jnp.int32)
    key_index = jnp.arange(rows, dtype=jnp.int32)
    my_seg = lax.dynamic_slice_in_dim(seg, start, mine, 0)
    allowed = (my_seg[:, None] == seg[None, :]) & (key_index[None, :] <= query_index[:, None])
    scores = jnp.where(allowed[None, None], scores, -1e30)
    top = jnp.max(scores, axis=-1, keepdims=True)
    expo = jnp.exp(scores - top)
    weights = (expo / jnp.sum(expo, axis=-1, keepdims=True)).astype(jnp.bfloat16)
    context = jnp.einsum("hgqk,khd->qhgd", weights, vals, preferred_element_type=jnp.float32)
    context = context.astype(jnp.bfloat16).reshape(mine, groups * share * HD)
    inner = lax.all_gather(policy_key, "rep", axis=0, tiled=True)
    outer = lax.all_gather(inner, "fsdp", axis=0, tiled=True)
    blocks = policy_key.shape[0]
    shards = outer.shape[0] // (blocks * replicas)
    whole = (
        outer.reshape(shards, replicas, blocks, outer.shape[1])
        .transpose(1, 0, 2, 3)
        .reshape(outer.shape)
    )
    return (context, whole)


def greet(devices, extra, condition):
    barrier = pltpu.get_barrier_semaphore()
    for device in devices:
        pl.semaphore_signal(barrier, inc=1, device_id=device, device_id_type=MESH)

    @pl.when(condition)
    def _():
        pl.semaphore_signal(barrier, inc=1, device_id=extra, device_id_type=MESH)
        pl.semaphore_wait(barrier, len(devices) + 1)

    @pl.when(jnp.logical_not(condition))
    def _():
        pl.semaphore_wait(barrier, len(devices))


class Copies:
    def __init__(self, send, recv, ring):
        self.send, self.recv, self.ring = send, recv, ring
        self.made, self.done, self.left, self.used = [], 0, set(), 0

    def place(self):
        self.used += 1
        return self.used - 1

    def start(self, src, dst, device, sends=None, place=None):
        n = len(self.made)
        self.retire(n - self.ring + 1)
        place = self.place() if place is None else place
        copy = pltpu.make_async_remote_copy(
            src_ref=src, dst_ref=dst, send_sem=self.send.at[n % self.ring], recv_sem=self.recv.at[place],
            device_id=device, device_id_type=MESH,
        )
        only(sends, copy.start)
        self.made.append((copy, sends))
        return copy

    def arrival(self, ref, device, place):
        return pltpu.make_async_remote_copy(
            src_ref=ref, dst_ref=ref, send_sem=self.send.at[0], recv_sem=self.recv.at[place],
            device_id=device, device_id_type=MESH,
        )

    def sent(self, n):
        if n not in self.left:
            self.left.add(n)
            copy, sends = self.made[n]
            only(sends, copy.wait_send)

    def retire(self, count):
        while self.done < count:
            self.sent(self.done)
            self.done += 1


def only(condition, act):
    if condition is None:
        act()
    else:
        pl.when(condition)(act)


def sizes_of(g, groups, share):
    if g == groups - 1:
        return [2] * (share // 2) + [1] * (share % 2)
    return [share - share // 2, share // 2]


def plan(groups, share):
    width = (share + 2) * HD
    pieces = []
    for g in range(groups):
        pair = [("k", g, share), ("v", g, share + 1)]
        pieces += [pair[:1], pair[1:]] if g == 0 else [pair]
    for g in range(groups):
        at = 0
        for size in sizes_of(g, groups, share):
            pieces.append([("q", g, j) for j in range(at, at + size)])
            at += size
    return [(heads[0][1] * width + heads[0][2] * HD, heads) for heads in pieces]


def layer_kernel(
    tok, w, bias, seg, pol, out, pg,
    x, wg, own, fin, snd, inb, kv, shut, cosine, sine, ctx, pv,
    send, recv, w_local, local, z_send, z_recv,
):
    f, r, t = lax.axis_index("fsdp"), lax.axis_index("rep"), lax.axis_index("tp")
    mine = x.shape[0] // 4
    block, columns = w.shape
    hb = block // 2
    share = QH // KVH
    width = (share + 2) * HD
    groups = columns // width
    fx = f + 1 - 2 * lax.rem(f, 2)
    fy = lax.rem(f + 2, 4)
    near = r + 1 - 2 * lax.rem(r, 2)
    across = 3 - r
    end = (r == 0) | (r == 3)
    mid = (r == 1) | (r == 2)
    to_x, to_y, to_near, to_across = {"fsdp": fx}, {"fsdp": fy}, {"rep": near}, {"rep": across}
    to_up, to_down = {"rep": lax.rem(r + 1, 4)}, {"rep": lax.rem(r + 3, 4)}
    copies = Copies(send, recv, RING)

    chunks = plan(groups, share)
    n = len(chunks)
    wide = [len(heads) * HD for _, heads in chunks]
    col = [pl.ds(at, wide[c]) for c, (at, _) in enumerate(chunks)]

    my_rows = pl.ds(pl.multiple_of(f * block, 16), block)
    parts = col[:2] + [pl.ds(width, columns - width), pl.ds(0, share * HD)]
    load_w = [pltpu.make_async_copy(w.at[:, at], wg.at[my_rows, at], w_local.at[i]) for i, at in enumerate(parts)]
    for copy in load_w:
        copy.start()
    loaded = set()
    load_x = pltpu.make_async_copy(tok, x, local.at[0])
    load_p = pltpu.make_async_copy(pol, pv, local.at[1])
    load_p.start()
    load_x.start()
    greet([to_x, to_y, to_near], to_across, mid)

    def held(owner, first, count, c):
        return wg.at[pl.ds(pl.multiple_of(owner * block + first, 16), count), col[c]]

    passed, onwards, last_direct, last_onward = {}, {}, {}, {}

    def direct(c):
        part = c if c < 2 else (3 if chunks[c][0] < width else 2)
        if part not in loaded:
            loaded.add(part)
            load_w[part].wait()
        src = held(f, 0, block, c)
        place = copies.place()
        last_direct[c] = len(copies.made)
        copies.start(src, src, to_x, place=place)
        copies.start(src, src, to_y, place=place)
        passed[c] = copies.arrival(wg.at[pl.ds(0, 2 * block), col[c]], to_x, place)

    def left(c):
        copies.sent(c)
        copies.sent(c + 1)

    def onward(c):
        passed[c].wait_recv()
        place = copies.place()
        copies.start(held(fx, 0, hb, c), held(fx, 0, hb, c), to_y, place=place)
        copies.start(held(fy, hb, hb, c), held(fy, hb, hb, c), to_x, place=place)
        last_onward[c] = len(copies.made) - 2
        onwards[c] = copies.arrival(wg.at[pl.ds(0, block), col[c]], to_x, place)

    def policy_at(j, owner, first=0, count=block):
        return pg.at[pl.ds(pl.multiple_of((j * 4 + owner) * block + first, 16), count)]

    p_up, p_down = {}, {}

    def policy_z(k):
        up_block, down_block = lax.rem(r + 5 - k, 4), lax.rem(r + k - 1, 4)
        up_src = pv if k == 1 else policy_at(up_block, f)
        down_src = pv if k == 1 else policy_at(down_block, f)
        if k > 1:
            landed_z(k - 1)
        p_up[k] = copies.start(up_src, policy_at(up_block, f), to_up, (r <= 2) & (r >= k - 1))
        p_down[k] = copies.start(down_src, policy_at(down_block, f), to_down, (r >= 1) & (r <= 4 - k))

    def landed_z(k):
        only(r >= k, p_up[k].wait_recv)
        only(r <= 3 - k, p_down[k].wait_recv)

    p_direct, p_onward = {}, {}

    def policy_direct(j):
        src, place = policy_at(j, f), copies.place()
        copies.start(src, src, to_x, place=place)
        copies.start(src, src, to_y, place=place)
        p_direct[j] = copies.arrival(pg.at[pl.ds(0, 2 * block)], to_x, place)

    def policy_onward(j):
        p_direct[j].wait_recv()
        place = copies.place()
        copies.start(policy_at(j, fx, 0, hb), policy_at(j, fx, 0, hb), to_y, place=place)
        copies.start(policy_at(j, fy, hb, hb), policy_at(j, fy, hb, hb), to_x, place=place)
        p_onward[j] = copies.arrival(pg.at[pl.ds(0, block)], to_x, place)

    def rows_of(slot):
        ahead = jnp.where(
            slot == 0, 3, jnp.where(slot == 1, 2, jnp.where((slot == 2) == end, 1, 0))
        )
        return jnp.where(r >= 2, 3 - ahead, ahead)

    def product(c, slot):
        rows = pl.ds(pl.multiple_of(rows_of(slot) * mine, mine), mine)
        return jnp.dot(x[rows, :], wg[:, col[c]], preferred_element_type=jnp.float32)

    def hop(c, slot, place, device):
        return pltpu.make_async_remote_copy(
            src_ref=snd.at[slot, :, col[c]], dst_ref=inb.at[place, :, col[c]],
            send_sem=z_send.at[slot, c % HOPS], recv_sem=z_recv.at[z_place(place), c],
            device_id=device, device_id_type=MESH,
        )

    def z_place(place):
        return (0, 1, 3, 2, 3)[place]

    def came(c, place):
        hop(c, 0, place, to_near).wait_recv()

    def came_last(c):
        both = inb.at[pl.ds(0, 2), :, col[c]]
        pair = pltpu.make_async_remote_copy(
            src_ref=both, dst_ref=both, send_sem=z_send.at[0, 0], recv_sem=z_recv.at[3, c],
            device_id=to_near, device_id_type=MESH,
        )
        pl.when(mid)(pair.wait_recv)
        pl.when(end)(hop(c, 0, 2, to_near).wait_recv)

    def work_end(*several):
        def one(slot, _):
            for c in several:
                snd[slot, :, col[c]] = product(c, slot).astype(jnp.bfloat16)
                pltpu.make_async_remote_copy(
                    src_ref=snd.at[slot, :, col[c]], dst_ref=inb.at[slot, :, col[c]],
                    send_sem=z_send.at[slot, c % HOPS], recv_sem=z_recv.at[jnp.where(slot == 2, 3, slot), c],
                    device_id=to_near, device_id_type=MESH,
                ).start()
            return 0

        lax.fori_loop(0, 3, one, 0)
        for c in several:
            fin[:, col[c]] = product(c, 3)

    def work_mid(c):
        here = pl.ds(0, wide[c])

        def one(slot, _):
            own[slot_of(c), slot, :, here] = product(c, slot)
            return 0

        lax.fori_loop(0, 3, one, 0)
        fin[:, col[c]] = product(c, 3)

    def work_one(c):
        if c >= 1:
            work_back(c - 1)
        work_across(c)

    def work_two(c):
        work_across(c)
        if c >= 1:
            work_back(c - 1)

    def work_across(*several):
        for slot in range(2):
            for c in several:
                relay(c, slot, slot, 3 + slot, to_across)

    def last_one():
        work_back(n - 2)
        work_back(n - 1)
        relay(n - 2, 0, 0, 3, to_across)
        relay(n - 1, 0, 0, 3, to_across)
        finish(n - 4)
        relay(n - 2, 1, 1, 4, to_across)
        relay(n - 1, 1, 1, 4, to_across)

    def last_two():
        work_across(n - 2, n - 1)
        work_back(n - 3)

    def last_back():
        work_back(n - 2)
        work_back(n - 1)

    def relay(c, slot, source, place, device):
        came(c, source)
        total = own[slot_of(c), slot, :, pl.ds(0, wide[c])] + inb[source, :, col[c]].astype(jnp.float32)
        snd[slot, :, col[c]] = total.astype(jnp.bfloat16)
        hop(c, slot, place, device).start()

    def work_back(c):
        relay(c, 2, 3, 2, to_near)

    def slot_of(c):
        return c % 3

    def summed(at):
        return (
            fin[:, at] + inb[2, :, at].astype(jnp.float32)
            + inb[4, :, at].astype(jnp.float32) + bias[at][None, :]
        )

    def rotated(values):
        return values * cosine[...] + pltpu.roll(values, HD // 2, 1) * sine[...]

    kv_up, kv_on = {}, {}

    def stored(kind, g):
        return pl.ds((2 * g + (kind == "v")) * HD, HD)

    def span(c):
        _, heads = chunks[c]
        return pl.ds((2 * heads[0][1] + (heads[0][0] == "v")) * HD, wide[c])

    key_chunks = [c for c in range(n) if chunks[c][1][0][0] != "q"]
    low, middle, high = (pl.ds(k * mine, mine) for k in range(3))

    def finish_keys(c):
        at, heads = chunks[c]
        for kind, g, j in heads:
            values = summed(pl.ds(at + (j - heads[0][2]) * HD, HD))
            kv[high, stored(kind, g)] = (rotated(values) if kind == "k" else values).astype(jnp.bfloat16)
        kv_up[c] = copies.start(kv.at[high, span(c)], kv.at[middle, span(c)], to_up, r <= 2)

    def forward_keys(c):
        only(r >= 1, kv_up[c].wait_recv)
        kv_on[c] = copies.start(kv.at[middle, span(c)], kv.at[low, span(c)], to_up, mid)

    scale = 1.0 / math.sqrt(HD)
    keys_in = set()

    def attend(c):
        at, heads = chunks[c]
        _, g, first = heads[0]
        for k in key_chunks:
            if k not in keys_in and chunks[k][1][0][1] == g:
                keys_in.add(k)
                only(r >= 2, kv_on[k].wait_recv)
        kc, vc = stored("k", g), stored("v", g)
        base = (g * share + first) * HD

        def head(j, _):
            query = rotated(summed(pl.ds(pl.multiple_of(at + j * HD, HD), HD))).astype(jnp.bfloat16)
            scores = lax.dot_general(
                query, kv[:, kc], (((1,), (1,)), ((), ())), preferred_element_type=jnp.float32
            ) * scale + shut[...]
            expo = jnp.exp(scores - jnp.max(scores, axis=-1, keepdims=True))
            total = jnp.sum(expo, axis=-1, keepdims=True)
            weights = (expo * (1.0 / total)).astype(jnp.bfloat16)
            to = pl.ds(pl.multiple_of(base + j * HD, HD), HD)
            ctx[:, to] = jnp.dot(weights, kv[:, vc], preferred_element_type=jnp.float32).astype(jnp.bfloat16)
            return 0

        lax.fori_loop(0, len(heads), head, 0)
        part = pl.ds(base, wide[c])
        pltpu.make_async_copy(ctx.at[:, part], out.at[:, part], local.at[3]).start()

    def finish(c):
        came_last(c)
        (attend if chunks[c][1][0][0] == "q" else finish_keys)(c)

    def prepare():
        at = pl.ds(pl.multiple_of(r * mine, mine), mine)
        square = (mine, mine)
        row, lane = lax.broadcasted_iota(jnp.int32, square, 0), lax.broadcasted_iota(jnp.int32, square, 1)
        mine_row = jnp.broadcast_to(seg[:, at].astype(jnp.float32), square)
        my_seg = jnp.sum(jnp.where(row == lane, mine_row, 0.0), axis=-1, keepdims=True)
        before = jnp.where(seg[...].astype(jnp.float32) < my_seg, 1.0, 0.0)
        first = jnp.sum(before, axis=-1, keepdims=True)
        index = lax.broadcasted_iota(jnp.int32, (mine, HD), 0) + r * mine
        half = HD // 2
        place = lax.rem(lax.broadcasted_iota(jnp.int32, (1, HD), 1), half)
        freq = jnp.ones((1, HD), jnp.float32)
        for i in range(1, half):
            freq = jnp.where(place == i, 1000000.0 ** (-2.0 * i / HD), freq)
        angle = (index.astype(jnp.float32) - first) * freq
        cosine[...] = jnp.cos(angle)
        wave = jnp.sin(angle)
        sine[...] = jnp.where(lax.broadcasted_iota(jnp.int32, (mine, HD), 1) < half, -wave, wave)
        for slot in range(3):
            there = r - 2 + slot
            keys = pl.ds(pl.multiple_of(jnp.maximum(there, 0) * mine, mine), mine)
            allowed = (my_seg == seg[:, keys].astype(jnp.float32)) & (there >= 0)
            if slot == 2:
                allowed = allowed & (lane <= row)
            shut[:, slot * mine:(slot + 1) * mine] = jnp.where(allowed, 0.0, -1e30)

        @pl.when(r <= 1)
        def _():
            kv[low, :] = jnp.zeros((mine, kv.shape[1]), kv.dtype)

        @pl.when(r == 0)
        def _():
            kv[middle, :] = jnp.zeros((mine, kv.shape[1]), kv.dtype)

        @pl.when(end)
        def _():
            inb[4] = jnp.zeros(inb.shape[1:], inb.dtype)

    def weights_in(c):
        onwards[c].wait_recv()

    queries = len(key_chunks)
    direct(0)
    load_p.wait()
    policy_z(1)
    keep_p = pltpu.make_async_copy(pv, policy_at(r, f), local.at[2])
    keep_p.start()
    left(last_direct[0])
    direct(1)
    onward(0)
    onward(1)
    load_x.wait()
    weights_in(0)
    direct(2)
    pl.when(end)(functools.partial(work_end, 0))
    policy_steps = {
        queries - 1: [("d", 0)], queries: [("d", 1)], queries + 1: [("o", 0), ("d", 2)], queries + 2: [("o", 1)],
        queries + 3: [("d", 3), ("o", 2)], queries + 5: [("o", 3)],
    }

    weight_steps = {0: "o2 d3", 1: "o3 d4", 2: "o4 d5", 3: "o5 d6 d7", 4: "o6 o7 d8 d9"}

    def weights_on(c):
        for word in weight_steps.get(c, f"o{c + 3} d{c + 5}").split():
            if int(word[1:]) < n:
                (direct if word[0] == "d" else onward)(int(word[1:]))

    def sends_out(c):
        for slot in range(3):
            hop(c, slot, 0, to_near).wait_send()

    for c in range(n - 2):
        ahead = [c + 1] if c < n - 3 else [n - 2, n - 1]
        for k in ahead:
            if k >= HOPS:
                sends_out(k - HOPS)
        if 0 <= c - 4 < queries:
            forward_keys(c - 4)
        early = c - 2 < queries - 2
        if 0 <= c - 2 < queries and not early:
            finish(c - 2)
        for k in ahead:
            weights_in(k)
        pl.when(end)(functools.partial(work_end, *ahead))
        if 0 <= c - 2 and early:
            finish(c - 2)
        if c < 3:
            weights_on(c)
        if c == 0:
            prepare()
            policy_z(2)
        if c == 2:
            policy_z(3)
        pl.when(mid)(functools.partial(work_mid, c))
        pl.when(r == 1)(functools.partial(work_one, c))
        pl.when(r == 2)(functools.partial(work_two, c))
        if c == n - 3:
            for k in ahead:
                pl.when(mid)(functools.partial(work_mid, k))
            pl.when(r == 1)(functools.partial(work_back, c))
        if c >= 3:
            weights_on(c)
        if c == queries - 1:
            landed_z(3)
            keep_p.wait()
        for kind, j in policy_steps.get(c, ()):
            (policy_direct if kind == "d" else policy_onward)(j)
        if queries <= c - 2:
            finish(c - 2)
    pl.when(r == 1)(last_one)
    pl.when(r == 2)(last_two)
    pl.when(r != 1)(functools.partial(finish, n - 4))
    finish(n - 3)
    pl.when(r == 2)(last_back)
    finish(n - 2)
    finish(n - 1)
    for j in range(4):
        p_onward[j].wait_recv()
    for c in range(n - HOPS, n):
        sends_out(c)
    copies.retire(len(copies.made))
    pltpu.make_async_copy(ctx, out, local.at[3]).wait()


def settle_kernel(ctx, pg, out, whole, store):
    step = pg.shape[0] // PIECES
    stores = [(pg.at[pl.ds(k * step, step)], whole.at[pl.ds(k * step, step)]) for k in range(PIECES)] + [(ctx, out)]
    stores = [pltpu.make_async_copy(src, dst, store.at[i]) for i, (src, dst) in enumerate(stores)]
    for copy in stores:
        copy.start()
    for copy in stores:
        copy.wait()


def whole_layer(tokens, ref_qkv, ref_bias, segment_ids, policy_key):
    rows, depth = tokens.shape
    block, columns = ref_qkv.shape
    mine, share = rows // 4, QH // KVH
    groups = columns // ((share + 2) * HD)
    chunks = plan(groups, share)
    n = len(chunks)
    keys = sum(heads[0][0] != "q" for _, heads in chunks)
    widest = max(len(heads) for _, heads in chunks) * HD
    places = 2 * n + 6 + 2 * keys + 8
    hbm, vmem = pl.BlockSpec(memory_space=pltpu.HBM), pl.BlockSpec(memory_space=pltpu.VMEM)
    any_space = pl.BlockSpec(memory_space=pl.ANY)
    low, full = jnp.bfloat16, jnp.float32
    dma = pltpu.SemaphoreType.DMA
    out, pg = pl.pallas_call(
        layer_kernel,
        out_shape=(
            pltpu.VMEM((mine, groups * share * HD), low),
            pltpu.VMEM((16 * block, policy_key.shape[1]), policy_key.dtype),
        ),
        in_specs=[hbm, hbm, vmem, vmem, hbm],
        out_specs=(any_space, any_space),
        scratch_shapes=[
            pltpu.VMEM((rows, depth), tokens.dtype),
            pltpu.VMEM((4 * block, columns), ref_qkv.dtype),
            pltpu.VMEM((3, 3, mine, widest), full),
            pltpu.VMEM((mine, columns), full),
            pltpu.VMEM((3, mine, columns), low),
            pltpu.VMEM((5, mine, columns), low),
            pltpu.VMEM((3 * mine, groups * 2 * HD), low),
            pltpu.VMEM((mine, 3 * mine), full),
            pltpu.VMEM((mine, HD), full),
            pltpu.VMEM((mine, HD), full),
            pltpu.VMEM((mine, groups * share * HD), low),
            pltpu.VMEM(policy_key.shape, policy_key.dtype),
            dma((RING,)),
            dma((places,)),
            dma((4,)),
            dma((4,)),
            dma((3, HOPS)),
            dma((4, n)),
        ],
        compiler_params=pltpu.CompilerParams(
            collective_id=0, has_side_effects=True, vmem_limit_bytes=VMEM_LIMIT
        ),
    )(tokens, ref_qkv, ref_bias, segment_ids, policy_key)
    return pl.pallas_call(
        settle_kernel,
        out_shape=tuple(jax.ShapeDtypeStruct(a.shape, a.dtype) for a in (out, pg)),
        in_specs=[any_space] * 2,
        out_specs=(any_space,) * 2,
        scratch_shapes=[dma((PIECES + 1,))],
        compiler_params=pltpu.CompilerParams(vmem_limit_bytes=VMEM_LIMIT),
    )(*(pltpu.with_memory_space_constraint(a, pltpu.VMEM) for a in (out, pg)))


PIECES = 4
VMEM_LIMIT = 50 * 1024 * 1024
RING = 32
HOPS = 4


def solution(mesh):
    in_specs = (
        P("fsdp", "rep"),
        P(("rep", "fsdp"), "tp"),
        P("tp"),
        P("fsdp", None),
        P(("rep", "fsdp"), "tp"),
    )
    out_specs = (P(("fsdp", "rep"), "tp"), P(None, "tp"))
    shape = mesh.shape
    grouped = shape["rep"] == 4 and shape["fsdp"] == 4 and shape["tp"] == 2
    return jax.shard_map(
        whole_layer if grouped else per_device, mesh=mesh, in_specs=in_specs, out_specs=out_specs, check_vma=False
    )
```

```python
import jax
import jax.numpy as jnp
from jax import lax
from jax.experimental import pallas as pl
from jax.experimental.pallas import tpu as pltpu
from jax.sharding import PartitionSpec as P
import functools
import math

MESH = pl.DeviceIdType.MESH

QH = 40
KVH = 8
HD = 128


def positions_of(seg):
    count = seg.shape[0]
    index = jnp.arange(count, dtype=jnp.int32)
    starts = jnp.concatenate([jnp.ones((1,), bool), seg[1:] != seg[:-1]])
    first = lax.cummax(jnp.where(starts, index, 0), axis=0)
    return index - first


def rotary(values, pos):
    half = values.shape[-1] // 2
    freq = 1000000.0 ** (-2.0 * jnp.arange(half, dtype=jnp.float32) / values.shape[-1])
    angle = pos.astype(jnp.float32)[:, None] * freq[None, :]
    shape = (values.shape[0],) + (1,) * (values.ndim - 2) + (half,)
    cosine = jnp.cos(angle).reshape(shape)
    sine = jnp.sin(angle).reshape(shape)
    first = values[..., :half]
    second = values[..., half:]
    return jnp.concatenate(
        [first * cosine - second * sine, second * cosine + first * sine], axis=-1
    )


def per_device(tokens, ref_qkv, ref_bias, segment_ids, policy_key):
    share = QH // KVH
    rows = tokens.shape[0]
    columns = ref_qkv.shape[1]
    groups = columns // ((share + 2) * HD)
    replicas = lax.axis_size("rep")
    mine = rows // replicas
    rank = lax.axis_index("rep")
    partial_value = jnp.dot(
        tokens,
        lax.all_gather(ref_qkv, "fsdp", axis=0, tiled=True),
        preferred_element_type=jnp.float32,
    )
    partial_value = partial_value.reshape(rows, groups, share + 2, HD)
    bias = ref_bias.reshape(groups, share + 2, HD)
    seg = segment_ids[0]
    pos = positions_of(seg)
    start = rank * mine
    my_pos = lax.dynamic_slice_in_dim(pos, start, mine, 0)
    summed = lax.psum_scatter(partial_value, "rep", scatter_dimension=0, tiled=True) + bias[None]
    query = rotary(summed[:, :, :share], my_pos).astype(jnp.bfloat16)
    my_keys = rotary(summed[:, :, share], my_pos).astype(jnp.bfloat16)
    my_vals = summed[:, :, share + 1].astype(jnp.bfloat16)
    keys, vals = (
        lax.all_gather(my_keys, "rep", axis=0, tiled=True),
        lax.all_gather(my_vals, "rep", axis=0, tiled=True),
    )
    scores = jnp.einsum(
        "qhgd,khd->hgqk", query, keys, preferred_element_type=jnp.float32
    ) / jnp.sqrt(jnp.float32(HD))
    query_index = start + jnp.arange(mine, dtype=jnp.int32)
    key_index = jnp.arange(rows, dtype=jnp.int32)
    my_seg = lax.dynamic_slice_in_dim(seg, start, mine, 0)
    allowed = (my_seg[:, None] == seg[None, :]) & (key_index[None, :] <= query_index[:, None])
    scores = jnp.where(allowed[None, None], scores, -1e30)
    top = jnp.max(scores, axis=-1, keepdims=True)
    expo = jnp.exp(scores - top)
    weights = (expo / jnp.sum(expo, axis=-1, keepdims=True)).astype(jnp.bfloat16)
    context = jnp.einsum("hgqk,khd->qhgd", weights, vals, preferred_element_type=jnp.float32)
    context = context.astype(jnp.bfloat16).reshape(mine, groups * share * HD)
    inner = lax.all_gather(policy_key, "rep", axis=0, tiled=True)
    outer = lax.all_gather(inner, "fsdp", axis=0, tiled=True)
    blocks = policy_key.shape[0]
    shards = outer.shape[0] // (blocks * replicas)
    whole = (
        outer.reshape(shards, replicas, blocks, outer.shape[1])
        .transpose(1, 0, 2, 3)
        .reshape(outer.shape)
    )
    return (context, whole)


def greet(devices, extra, condition):
    barrier = pltpu.get_barrier_semaphore()
    for device in devices:
        pl.semaphore_signal(barrier, inc=1, device_id=device, device_id_type=MESH)

    @pl.when(condition)
    def _():
        pl.semaphore_signal(barrier, inc=1, device_id=extra, device_id_type=MESH)
        pl.semaphore_wait(barrier, len(devices) + 1)

    @pl.when(jnp.logical_not(condition))
    def _():
        pl.semaphore_wait(barrier, len(devices))


class Copies:
    def __init__(self, send, recv, ring):
        self.send, self.recv, self.ring = send, recv, ring
        self.made, self.done, self.left, self.used = [], 0, set(), 0

    def place(self):
        self.used += 1
        return self.used - 1

    def start(self, src, dst, device, sends=None, place=None):
        n = len(self.made)
        self.retire(n - self.ring + 1)
        place = self.place() if place is None else place
        copy = pltpu.make_async_remote_copy(
            src_ref=src, dst_ref=dst, send_sem=self.send.at[n % self.ring], recv_sem=self.recv.at[place],
            device_id=device, device_id_type=MESH,
        )
        only(sends, copy.start)
        self.made.append((copy, sends))
        return copy

    def arrival(self, ref, device, place):
        return pltpu.make_async_remote_copy(
            src_ref=ref, dst_ref=ref, send_sem=self.send.at[0], recv_sem=self.recv.at[place],
            device_id=device, device_id_type=MESH,
        )

    def sent(self, n):
        if n not in self.left:
            self.left.add(n)
            copy, sends = self.made[n]
            only(sends, copy.wait_send)

    def retire(self, count):
        while self.done < count:
            self.sent(self.done)
            self.done += 1


def only(condition, act):
    if condition is None:
        act()
    else:
        pl.when(condition)(act)


def sizes_of(g, groups, share):
    if g == groups - 1:
        return [2] * (share // 2) + [1] * (share % 2)
    return [share - share // 2, share // 2]


def plan(groups, share):
    width = (share + 2) * HD
    pieces = []
    for g in range(groups):
        pair = [("k", g, share), ("v", g, share + 1)]
        pieces += [pair[:1], pair[1:]] if g == 0 else [pair]
    for g in range(groups):
        at = 0
        for size in sizes_of(g, groups, share):
            pieces.append([("q", g, j) for j in range(at, at + size)])
            at += size
    return [(heads[0][1] * width + heads[0][2] * HD, heads) for heads in pieces]


def layer_kernel(
    tok, w, bias, seg, pol, out, pg,
    x, wg, own, fin, snd, inb, kv, shut, cosine, sine, ctx, pv,
    send, recv, w_local, local, z_send, z_recv,
):
    f, r, t = lax.axis_index("fsdp"), lax.axis_index("rep"), lax.axis_index("tp")
    mine = x.shape[0] // 4
    block, columns = w.shape
    hb = block // 2
    share = QH // KVH
    width = (share + 2) * HD
    groups = columns // width
    fx = f + 1 - 2 * lax.rem(f, 2)
    fy = lax.rem(f + 2, 4)
    near = r + 1 - 2 * lax.rem(r, 2)
    across = 3 - r
    end = (r == 0) | (r == 3)
    mid = (r == 1) | (r == 2)
    to_x, to_y, to_near, to_across = {"fsdp": fx}, {"fsdp": fy}, {"rep": near}, {"rep": across}
    to_up, to_down = {"rep": lax.rem(r + 1, 4)}, {"rep": lax.rem(r + 3, 4)}
    copies = Copies(send, recv, RING)

    chunks = plan(groups, share)
    n = len(chunks)
    wide = [len(heads) * HD for _, heads in chunks]
    col = [pl.ds(at, wide[c]) for c, (at, _) in enumerate(chunks)]

    my_rows = pl.ds(pl.multiple_of(f * block, 16), block)
    parts = col[:2] + [pl.ds(width, columns - width), pl.ds(0, share * HD)]
    load_w = [pltpu.make_async_copy(w.at[:, at], wg.at[my_rows, at], w_local.at[i]) for i, at in enumerate(parts)]
    for copy in load_w:
        copy.start()
    loaded = set()
    load_x = pltpu.make_async_copy(tok, x, local.at[0])
    load_p = pltpu.make_async_copy(pol, pv, local.at[1])
    load_p.start()
    load_x.start()
    greet([to_x, to_y, to_near], to_across, mid)

    def held(owner, first, count, c):
        return wg.at[pl.ds(pl.multiple_of(owner * block + first, 16), count), col[c]]

    passed, onwards, last_direct, last_onward = {}, {}, {}, {}

    def direct(c):
        part = c if c < 2 else (3 if chunks[c][0] < width else 2)
        if part not in loaded:
            loaded.add(part)
            load_w[part].wait()
        src = held(f, 0, block, c)
        place = copies.place()
        last_direct[c] = len(copies.made)
        copies.start(src, src, to_x, place=place)
        copies.start(src, src, to_y, place=place)
        passed[c] = copies.arrival(wg.at[pl.ds(0, 2 * block), col[c]], to_x, place)

    def left(c):
        copies.sent(c)
        copies.sent(c + 1)

    def onward(c):
        passed[c].wait_recv()
        place = copies.place()
        copies.start(held(fx, 0, hb, c), held(fx, 0, hb, c), to_y, place=place)
        copies.start(held(fy, hb, hb, c), held(fy, hb, hb, c), to_x, place=place)
        last_onward[c] = len(copies.made) - 2
        onwards[c] = copies.arrival(wg.at[pl.ds(0, block), col[c]], to_x, place)

    def policy_at(j, owner, first=0, count=block):
        return pg.at[pl.ds(pl.multiple_of((j * 4 + owner) * block + first, 16), count)]

    p_up, p_down = {}, {}

    def policy_z(k):
        up_block, down_block = lax.rem(r + 5 - k, 4), lax.rem(r + k - 1, 4)
        up_src = pv if k == 1 else policy_at(up_block, f)
        down_src = pv if k == 1 else policy_at(down_block, f)
        if k > 1:
            landed_z(k - 1)
        p_up[k] = copies.start(up_src, policy_at(up_block, f), to_up, (r <= 2) & (r >= k - 1))
        p_down[k] = copies.start(down_src, policy_at(down_block, f), to_down, (r >= 1) & (r <= 4 - k))

    def landed_z(k):
        only(r >= k, p_up[k].wait_recv)
        only(r <= 3 - k, p_down[k].wait_recv)

    p_direct, p_onward = {}, {}

    def policy_direct(j):
        src, place = policy_at(j, f), copies.place()
        copies.start(src, src, to_x, place=place)
        copies.start(src, src, to_y, place=place)
        p_direct[j] = copies.arrival(pg.at[pl.ds(0, 2 * block)], to_x, place)

    def policy_onward(j):
        p_direct[j].wait_recv()
        place = copies.place()
        copies.start(policy_at(j, fx, 0, hb), policy_at(j, fx, 0, hb), to_y, place=place)
        copies.start(policy_at(j, fy, hb, hb), policy_at(j, fy, hb, hb), to_x, place=place)
        p_onward[j] = copies.arrival(pg.at[pl.ds(0, block)], to_x, place)

    def rows_of(slot):
        ahead = jnp.where(
            slot == 0, 3, jnp.where(slot == 1, 2, jnp.where((slot == 2) == end, 1, 0))
        )
        return jnp.where(r >= 2, 3 - ahead, ahead)

    def product(c, slot):
        rows = pl.ds(pl.multiple_of(rows_of(slot) * mine, mine), mine)
        return jnp.dot(x[rows, :], wg[:, col[c]], preferred_element_type=jnp.float32)

    def hop(c, slot, place, device):
        return pltpu.make_async_remote_copy(
            src_ref=snd.at[slot, :, col[c]], dst_ref=inb.at[place, :, col[c]],
            send_sem=z_send.at[slot, c % HOPS], recv_sem=z_recv.at[z_place(place), c],
            device_id=device, device_id_type=MESH,
        )

    def z_place(place):
        return (0, 1, 3, 2, 3)[place]

    def came(c, place):
        hop(c, 0, place, to_near).wait_recv()

    def came_last(c):
        both = inb.at[pl.ds(0, 2), :, col[c]]
        pair = pltpu.make_async_remote_copy(
            src_ref=both, dst_ref=both, send_sem=z_send.at[0, 0], recv_sem=z_recv.at[3, c],
            device_id=to_near, device_id_type=MESH,
        )
        pl.when(mid)(pair.wait_recv)
        pl.when(end)(hop(c, 0, 2, to_near).wait_recv)

    def work_end(*several):
        def one(slot, _):
            for c in several:
                snd[slot, :, col[c]] = product(c, slot).astype(jnp.bfloat16)
                pltpu.make_async_remote_copy(
                    src_ref=snd.at[slot, :, col[c]], dst_ref=inb.at[slot, :, col[c]],
                    send_sem=z_send.at[slot, c % HOPS], recv_sem=z_recv.at[jnp.where(slot == 2, 3, slot), c],
                    device_id=to_near, device_id_type=MESH,
                ).start()
            return 0

        lax.fori_loop(0, 3, one, 0)
        for c in several:
            fin[:, col[c]] = product(c, 3)

    def work_mid(c):
        here = pl.ds(0, wide[c])

        def one(slot, _):
            own[slot_of(c), slot, :, here] = product(c, slot)
            return 0

        lax.fori_loop(0, 3, one, 0)
        fin[:, col[c]] = product(c, 3)

    def work_one(c):
        if c >= 1:
            work_back(c - 1)
        work_across(c)

    def work_two(c):
        work_across(c)
        if c >= 1:
            work_back(c - 1)

    def work_across(*several):
        for slot in range(2):
            for c in several:
                relay(c, slot, slot, 3 + slot, to_across)

    def last_one():
        relay(n - 2, 0, 0, 3, to_across)
        relay(n - 1, 0, 0, 3, to_across)
        work_back(n - 2)
        work_back(n - 1)
        finish(n - 4)
        relay(n - 2, 1, 1, 4, to_across)
        relay(n - 1, 1, 1, 4, to_across)

    def last_two():
        work_across(n - 2, n - 1)
        work_back(n - 3)

    def last_back():
        work_back(n - 2)
        work_back(n - 1)

    def relay(c, slot, source, place, device):
        came(c, source)
        total = own[slot_of(c), slot, :, pl.ds(0, wide[c])] + inb[source, :, col[c]].astype(jnp.float32)
        snd[slot, :, col[c]] = total.astype(jnp.bfloat16)
        hop(c, slot, place, device).start()

    def work_back(c):
        relay(c, 2, 3, 2, to_near)

    def slot_of(c):
        return c % 3

    def summed(at):
        return (
            fin[:, at] + inb[2, :, at].astype(jnp.float32)
            + inb[4, :, at].astype(jnp.float32) + bias[at][None, :]
        )

    def rotated(values):
        return values * cosine[...] + pltpu.roll(values, HD // 2, 1) * sine[...]

    kv_up, kv_on = {}, {}

    def stored(kind, g):
        return pl.ds((2 * g + (kind == "v")) * HD, HD)

    def span(c):
        _, heads = chunks[c]
        return pl.ds((2 * heads[0][1] + (heads[0][0] == "v")) * HD, wide[c])

    key_chunks = [c for c in range(n) if chunks[c][1][0][0] != "q"]
    low, middle, high = (pl.ds(k * mine, mine) for k in range(3))

    def finish_keys(c):
        at, heads = chunks[c]
        for kind, g, j in heads:
            values = summed(pl.ds(at + (j - heads[0][2]) * HD, HD))
            kv[high, stored(kind, g)] = (rotated(values) if kind == "k" else values).astype(jnp.bfloat16)
        kv_up[c] = copies.start(kv.at[high, span(c)], kv.at[middle, span(c)], to_up, r <= 2)

    def forward_keys(c):
        only(r >= 1, kv_up[c].wait_recv)
        kv_on[c] = copies.start(kv.at[middle, span(c)], kv.at[low, span(c)], to_up, mid)

    scale = 1.0 / math.sqrt(HD)
    keys_in = set()

    def attend(c):
        at, heads = chunks[c]
        _, g, first = heads[0]
        for k in key_chunks:
            if k not in keys_in and chunks[k][1][0][1] == g:
                keys_in.add(k)
                only(r >= 2, kv_on[k].wait_recv)
        kc, vc = stored("k", g), stored("v", g)
        base = (g * share + first) * HD

        def head(j, _):
            query = rotated(summed(pl.ds(pl.multiple_of(at + j * HD, HD), HD))).astype(jnp.bfloat16)
            scores = lax.dot_general(
                query, kv[:, kc], (((1,), (1,)), ((), ())), preferred_element_type=jnp.float32
            ) * scale + shut[...]
            expo = jnp.exp(scores - jnp.max(scores, axis=-1, keepdims=True))
            total = jnp.sum(expo, axis=-1, keepdims=True)
            weights = (expo * (1.0 / total)).astype(jnp.bfloat16)
            to = pl.ds(pl.multiple_of(base + j * HD, HD), HD)
            ctx[:, to] = jnp.dot(weights, kv[:, vc], preferred_element_type=jnp.float32).astype(jnp.bfloat16)
            return 0

        lax.fori_loop(0, len(heads), head, 0)
        part = pl.ds(base, wide[c])
        pltpu.make_async_copy(ctx.at[:, part], out.at[:, part], local.at[3]).start()

    def finish(c):
        came_last(c)
        (attend if chunks[c][1][0][0] == "q" else finish_keys)(c)

    def prepare():
        at = pl.ds(pl.multiple_of(r * mine, mine), mine)
        square = (mine, mine)
        row, lane = lax.broadcasted_iota(jnp.int32, square, 0), lax.broadcasted_iota(jnp.int32, square, 1)
        mine_row = jnp.broadcast_to(seg[:, at].astype(jnp.float32), square)
        my_seg = jnp.sum(jnp.where(row == lane, mine_row, 0.0), axis=-1, keepdims=True)
        before = jnp.where(seg[...].astype(jnp.float32) < my_seg, 1.0, 0.0)
        first = jnp.sum(before, axis=-1, keepdims=True)
        index = lax.broadcasted_iota(jnp.int32, (mine, HD), 0) + r * mine
        half = HD // 2
        place = lax.rem(lax.broadcasted_iota(jnp.int32, (1, HD), 1), half)
        freq = jnp.ones((1, HD), jnp.float32)
        for i in range(1, half):
            freq = jnp.where(place == i, 1000000.0 ** (-2.0 * i / HD), freq)
        angle = (index.astype(jnp.float32) - first) * freq
        cosine[...] = jnp.cos(angle)
        wave = jnp.sin(angle)
        sine[...] = jnp.where(lax.broadcasted_iota(jnp.int32, (mine, HD), 1) < half, -wave, wave)
        for slot in range(3):
            there = r - 2 + slot
            keys = pl.ds(pl.multiple_of(jnp.maximum(there, 0) * mine, mine), mine)
            allowed = (my_seg == seg[:, keys].astype(jnp.float32)) & (there >= 0)
            if slot == 2:
                allowed = allowed & (lane <= row)
            shut[:, slot * mine:(slot + 1) * mine] = jnp.where(allowed, 0.0, -1e30)

        @pl.when(r <= 1)
        def _():
            kv[low, :] = jnp.zeros((mine, kv.shape[1]), kv.dtype)

        @pl.when(r == 0)
        def _():
            kv[middle, :] = jnp.zeros((mine, kv.shape[1]), kv.dtype)

        @pl.when(end)
        def _():
            inb[4] = jnp.zeros(inb.shape[1:], inb.dtype)

    def weights_in(c):
        onwards[c].wait_recv()

    queries = len(key_chunks)
    direct(0)
    load_p.wait()
    policy_z(1)
    keep_p = pltpu.make_async_copy(pv, policy_at(r, f), local.at[2])
    keep_p.start()
    left(last_direct[0])
    direct(1)
    onward(0)
    onward(1)
    load_x.wait()
    weights_in(0)
    direct(2)
    pl.when(end)(functools.partial(work_end, 0))
    policy_steps = {
        queries - 1: [("d", 0)], queries: [("d", 1)], queries + 1: [("o", 0), ("d", 2)], queries + 2: [("o", 1)],
        queries + 3: [("d", 3), ("o", 2)], queries + 5: [("o", 3)],
    }

    weight_steps = {0: "o2 d3", 1: "o3 d4", 2: "o4 d5", 3: "o5 d6 d7", 4: "o6 o7 d8 d9"}

    def weights_on(c):
        for word in weight_steps.get(c, f"o{c + 3} d{c + 5}").split():
            if int(word[1:]) < n:
                (direct if word[0] == "d" else onward)(int(word[1:]))

    def sends_out(c):
        for slot in range(3):
            hop(c, slot, 0, to_near).wait_send()

    for c in range(n - 2):
        ahead = [c + 1] if c < n - 3 else [n - 2, n - 1]
        for k in ahead:
            if k >= HOPS:
                sends_out(k - HOPS)
        if 0 <= c - 4 < queries:
            forward_keys(c - 4)
        early = c - 2 < queries - 2
        if 0 <= c - 2 < queries and not early:
            finish(c - 2)
        for k in ahead:
            weights_in(k)
        pl.when(end)(functools.partial(work_end, *ahead))
        if 0 <= c - 2 and early:
            finish(c - 2)
        if c < 3:
            weights_on(c)
        if c == 0:
            prepare()
            policy_z(2)
        if c == 2:
            policy_z(3)
        pl.when(mid)(functools.partial(work_mid, c))
        pl.when(r == 1)(functools.partial(work_one, c))
        pl.when(r == 2)(functools.partial(work_two, c))
        if c == n - 3:
            for k in ahead:
                pl.when(mid)(functools.partial(work_mid, k))
            pl.when(r == 1)(functools.partial(work_back, c))
        if c >= 3:
            weights_on(c)
        if c == queries - 1:
            landed_z(3)
            keep_p.wait()
        for kind, j in policy_steps.get(c, ()):
            (policy_direct if kind == "d" else policy_onward)(j)
        if queries <= c - 2:
            finish(c - 2)
    pl.when(r == 1)(last_one)
    pl.when(r == 2)(last_two)
    pl.when(r != 1)(functools.partial(finish, n - 4))
    finish(n - 3)
    pl.when(r == 2)(last_back)
    finish(n - 2)
    finish(n - 1)
    for j in range(4):
        p_onward[j].wait_recv()
    for c in range(n - HOPS, n):
        sends_out(c)
    copies.retire(len(copies.made))
    pltpu.make_async_copy(ctx, out, local.at[3]).wait()


def settle_kernel(ctx, pg, out, whole, store):
    step = pg.shape[0] // PIECES
    stores = [(pg.at[pl.ds(k * step, step)], whole.at[pl.ds(k * step, step)]) for k in range(PIECES)] + [(ctx, out)]
    stores = [pltpu.make_async_copy(src, dst, store.at[i]) for i, (src, dst) in enumerate(stores)]
    for copy in stores:
        copy.start()
    for copy in stores:
        copy.wait()


def whole_layer(tokens, ref_qkv, ref_bias, segment_ids, policy_key):
    rows, depth = tokens.shape
    block, columns = ref_qkv.shape
    mine, share = rows // 4, QH // KVH
    groups = columns // ((share + 2) * HD)
    chunks = plan(groups, share)
    n = len(chunks)
    keys = sum(heads[0][0] != "q" for _, heads in chunks)
    widest = max(len(heads) for _, heads in chunks) * HD
    places = 2 * n + 6 + 2 * keys + 8
    hbm, vmem = pl.BlockSpec(memory_space=pltpu.HBM), pl.BlockSpec(memory_space=pltpu.VMEM)
    any_space = pl.BlockSpec(memory_space=pl.ANY)
    low, full = jnp.bfloat16, jnp.float32
    dma = pltpu.SemaphoreType.DMA
    out, pg = pl.pallas_call(
        layer_kernel,
        out_shape=(
            pltpu.VMEM((mine, groups * share * HD), low),
            pltpu.VMEM((16 * block, policy_key.shape[1]), policy_key.dtype),
        ),
        in_specs=[hbm, hbm, vmem, vmem, hbm],
        out_specs=(any_space, any_space),
        scratch_shapes=[
            pltpu.VMEM((rows, depth), tokens.dtype),
            pltpu.VMEM((4 * block, columns), ref_qkv.dtype),
            pltpu.VMEM((3, 3, mine, widest), full),
            pltpu.VMEM((mine, columns), full),
            pltpu.VMEM((3, mine, columns), low),
            pltpu.VMEM((5, mine, columns), low),
            pltpu.VMEM((3 * mine, groups * 2 * HD), low),
            pltpu.VMEM((mine, 3 * mine), full),
            pltpu.VMEM((mine, HD), full),
            pltpu.VMEM((mine, HD), full),
            pltpu.VMEM((mine, groups * share * HD), low),
            pltpu.VMEM(policy_key.shape, policy_key.dtype),
            dma((RING,)),
            dma((places,)),
            dma((4,)),
            dma((4,)),
            dma((3, HOPS)),
            dma((4, n)),
        ],
        compiler_params=pltpu.CompilerParams(
            collective_id=0, has_side_effects=True, vmem_limit_bytes=VMEM_LIMIT
        ),
    )(tokens, ref_qkv, ref_bias, segment_ids, policy_key)
    return pl.pallas_call(
        settle_kernel,
        out_shape=tuple(jax.ShapeDtypeStruct(a.shape, a.dtype) for a in (out, pg)),
        in_specs=[any_space] * 2,
        out_specs=(any_space,) * 2,
        scratch_shapes=[dma((PIECES + 1,))],
        compiler_params=pltpu.CompilerParams(vmem_limit_bytes=VMEM_LIMIT),
    )(*(pltpu.with_memory_space_constraint(a, pltpu.VMEM) for a in (out, pg)))


PIECES = 4
VMEM_LIMIT = 50 * 1024 * 1024
RING = 32
HOPS = 4


def solution(mesh):
    in_specs = (
        P("fsdp", "rep"),
        P(("rep", "fsdp"), "tp"),
        P("tp"),
        P("fsdp", None),
        P(("rep", "fsdp"), "tp"),
    )
    out_specs = (P(("fsdp", "rep"), "tp"), P(None, "tp"))
    shape = mesh.shape
    grouped = shape["rep"] == 4 and shape["fsdp"] == 4 and shape["tp"] == 2
    return jax.shard_map(
        whole_layer if grouped else per_device, mesh=mesh, in_specs=in_specs, out_specs=out_specs, check_vma=False
    )
```

```python
import jax
import jax.numpy as jnp
from jax import lax
from jax.experimental import pallas as pl
from jax.experimental.pallas import tpu as pltpu
from jax.sharding import PartitionSpec as P
import functools
import math

MESH = pl.DeviceIdType.MESH

QH = 40
KVH = 8
HD = 128


def positions_of(seg):
    count = seg.shape[0]
    index = jnp.arange(count, dtype=jnp.int32)
    starts = jnp.concatenate([jnp.ones((1,), bool), seg[1:] != seg[:-1]])
    first = lax.cummax(jnp.where(starts, index, 0), axis=0)
    return index - first


def rotary(values, pos):
    half = values.shape[-1] // 2
    freq = 1000000.0 ** (-2.0 * jnp.arange(half, dtype=jnp.float32) / values.shape[-1])
    angle = pos.astype(jnp.float32)[:, None] * freq[None, :]
    shape = (values.shape[0],) + (1,) * (values.ndim - 2) + (half,)
    cosine = jnp.cos(angle).reshape(shape)
    sine = jnp.sin(angle).reshape(shape)
    first = values[..., :half]
    second = values[..., half:]
    return jnp.concatenate(
        [first * cosine - second * sine, second * cosine + first * sine], axis=-1
    )


def per_device(tokens, ref_qkv, ref_bias, segment_ids, policy_key):
    share = QH // KVH
    rows = tokens.shape[0]
    columns = ref_qkv.shape[1]
    groups = columns // ((share + 2) * HD)
    replicas = lax.axis_size("rep")
    mine = rows // replicas
    rank = lax.axis_index("rep")
    partial_value = jnp.dot(
        tokens,
        lax.all_gather(ref_qkv, "fsdp", axis=0, tiled=True),
        preferred_element_type=jnp.float32,
    )
    partial_value = partial_value.reshape(rows, groups, share + 2, HD)
    bias = ref_bias.reshape(groups, share + 2, HD)
    seg = segment_ids[0]
    pos = positions_of(seg)
    start = rank * mine
    my_pos = lax.dynamic_slice_in_dim(pos, start, mine, 0)
    summed = lax.psum_scatter(partial_value, "rep", scatter_dimension=0, tiled=True) + bias[None]
    query = rotary(summed[:, :, :share], my_pos).astype(jnp.bfloat16)
    my_keys = rotary(summed[:, :, share], my_pos).astype(jnp.bfloat16)
    my_vals = summed[:, :, share + 1].astype(jnp.bfloat16)
    keys, vals = (
        lax.all_gather(my_keys, "rep", axis=0, tiled=True),
        lax.all_gather(my_vals, "rep", axis=0, tiled=True),
    )
    scores = jnp.einsum(
        "qhgd,khd->hgqk", query, keys, preferred_element_type=jnp.float32
    ) / jnp.sqrt(jnp.float32(HD))
    query_index = start + jnp.arange(mine, dtype=jnp.int32)
    key_index = jnp.arange(rows, dtype=jnp.int32)
    my_seg = lax.dynamic_slice_in_dim(seg, start, mine, 0)
    allowed = (my_seg[:, None] == seg[None, :]) & (key_index[None, :] <= query_index[:, None])
    scores = jnp.where(allowed[None, None], scores, -1e30)
    top = jnp.max(scores, axis=-1, keepdims=True)
    expo = jnp.exp(scores - top)
    weights = (expo / jnp.sum(expo, axis=-1, keepdims=True)).astype(jnp.bfloat16)
    context = jnp.einsum("hgqk,khd->qhgd", weights, vals, preferred_element_type=jnp.float32)
    context = context.astype(jnp.bfloat16).reshape(mine, groups * share * HD)
    inner = lax.all_gather(policy_key, "rep", axis=0, tiled=True)
    outer = lax.all_gather(inner, "fsdp", axis=0, tiled=True)
    blocks = policy_key.shape[0]
    shards = outer.shape[0] // (blocks * replicas)
    whole = (
        outer.reshape(shards, replicas, blocks, outer.shape[1])
        .transpose(1, 0, 2, 3)
        .reshape(outer.shape)
    )
    return (context, whole)


def greet(devices, extra, condition):
    barrier = pltpu.get_barrier_semaphore()
    for device in devices:
        pl.semaphore_signal(barrier, inc=1, device_id=device, device_id_type=MESH)

    @pl.when(condition)
    def _():
        pl.semaphore_signal(barrier, inc=1, device_id=extra, device_id_type=MESH)
        pl.semaphore_wait(barrier, len(devices) + 1)

    @pl.when(jnp.logical_not(condition))
    def _():
        pl.semaphore_wait(barrier, len(devices))


class Copies:
    def __init__(self, send, recv, ring):
        self.send, self.recv, self.ring = send, recv, ring
        self.made, self.done, self.left, self.used = [], 0, set(), 0

    def place(self):
        self.used += 1
        return self.used - 1

    def start(self, src, dst, device, sends=None, place=None):
        n = len(self.made)
        self.retire(n - self.ring + 1)
        place = self.place() if place is None else place
        copy = pltpu.make_async_remote_copy(
            src_ref=src, dst_ref=dst, send_sem=self.send.at[n % self.ring], recv_sem=self.recv.at[place],
            device_id=device, device_id_type=MESH,
        )
        only(sends, copy.start)
        self.made.append((copy, sends))
        return copy

    def arrival(self, ref, device, place):
        return pltpu.make_async_remote_copy(
            src_ref=ref, dst_ref=ref, send_sem=self.send.at[0], recv_sem=self.recv.at[place],
            device_id=device, device_id_type=MESH,
        )

    def sent(self, n):
        if n not in self.left:
            self.left.add(n)
            copy, sends = self.made[n]
            only(sends, copy.wait_send)

    def retire(self, count):
        while self.done < count:
            self.sent(self.done)
            self.done += 1


def only(condition, act):
    if condition is None:
        act()
    else:
        pl.when(condition)(act)


def sizes_of(g, groups, share):
    if g == groups - 1:
        return [2] * (share // 2) + [1] * (share % 2)
    return [share - share // 2, share // 2]


def plan(groups, share):
    width = (share + 2) * HD
    pieces = []
    for g in range(groups):
        pair = [("k", g, share), ("v", g, share + 1)]
        pieces += [pair[:1], pair[1:]] if g == 0 else [pair]
    for g in range(groups):
        at = 0
        for size in sizes_of(g, groups, share):
            pieces.append([("q", g, j) for j in range(at, at + size)])
            at += size
    return [(heads[0][1] * width + heads[0][2] * HD, heads) for heads in pieces]


def layer_kernel(
    tok, w, bias, seg, pol, out, pg,
    x, wg, own, fin, snd, inb, kv, shut, cosine, sine, ctx, pv,
    send, recv, w_local, local, z_send, z_recv,
):
    f, r, t = lax.axis_index("fsdp"), lax.axis_index("rep"), lax.axis_index("tp")
    mine = x.shape[0] // 4
    block, columns = w.shape
    hb = block // 2
    share = QH // KVH
    width = (share + 2) * HD
    groups = columns // width
    fx = f + 1 - 2 * lax.rem(f, 2)
    fy = lax.rem(f + 2, 4)
    near = r + 1 - 2 * lax.rem(r, 2)
    across = 3 - r
    end = (r == 0) | (r == 3)
    mid = (r == 1) | (r == 2)
    to_x, to_y, to_near, to_across = {"fsdp": fx}, {"fsdp": fy}, {"rep": near}, {"rep": across}
    to_up, to_down = {"rep": lax.rem(r + 1, 4)}, {"rep": lax.rem(r + 3, 4)}
    copies = Copies(send, recv, RING)

    chunks = plan(groups, share)
    n = len(chunks)
    wide = [len(heads) * HD for _, heads in chunks]
    col = [pl.ds(at, wide[c]) for c, (at, _) in enumerate(chunks)]

    my_rows = pl.ds(pl.multiple_of(f * block, 16), block)
    parts = col[:2] + [pl.ds(width, columns - width), pl.ds(0, share * HD)]
    load_w = [pltpu.make_async_copy(w.at[:, at], wg.at[my_rows, at], w_local.at[i]) for i, at in enumerate(parts)]
    for copy in load_w:
        copy.start()
    loaded = set()
    load_x = pltpu.make_async_copy(tok, x, local.at[0])
    load_p = pltpu.make_async_copy(pol, pv, local.at[1])
    load_p.start()
    load_x.start()
    greet([to_x, to_y, to_near], to_across, mid)

    def held(owner, first, count, c):
        return wg.at[pl.ds(pl.multiple_of(owner * block + first, 16), count), col[c]]

    passed, onwards, last_direct, last_onward = {}, {}, {}, {}

    def direct(c):
        part = c if c < 2 else (3 if chunks[c][0] < width else 2)
        if part not in loaded:
            loaded.add(part)
            load_w[part].wait()
        src = held(f, 0, block, c)
        place = copies.place()
        last_direct[c] = len(copies.made)
        copies.start(src, src, to_x, place=place)
        copies.start(src, src, to_y, place=place)
        passed[c] = copies.arrival(wg.at[pl.ds(0, 2 * block), col[c]], to_x, place)

    def left(c):
        copies.sent(c)
        copies.sent(c + 1)

    def onward(c):
        passed[c].wait_recv()
        place = copies.place()
        copies.start(held(fx, 0, hb, c), held(fx, 0, hb, c), to_y, place=place)
        copies.start(held(fy, hb, hb, c), held(fy, hb, hb, c), to_x, place=place)
        last_onward[c] = len(copies.made) - 2
        onwards[c] = copies.arrival(wg.at[pl.ds(0, block), col[c]], to_x, place)

    def policy_at(j, owner, first=0, count=block):
        return pg.at[pl.ds(pl.multiple_of((j * 4 + owner) * block + first, 16), count)]

    p_up, p_down = {}, {}

    def policy_z(k):
        up_block, down_block = lax.rem(r + 5 - k, 4), lax.rem(r + k - 1, 4)
        up_src = pv if k == 1 else policy_at(up_block, f)
        down_src = pv if k == 1 else policy_at(down_block, f)
        if k > 1:
            landed_z(k - 1)
        p_up[k] = copies.start(up_src, policy_at(up_block, f), to_up, (r <= 2) & (r >= k - 1))
        p_down[k] = copies.start(down_src, policy_at(down_block, f), to_down, (r >= 1) & (r <= 4 - k))

    def landed_z(k):
        only(r >= k, p_up[k].wait_recv)
        only(r <= 3 - k, p_down[k].wait_recv)

    p_direct, p_onward = {}, {}

    def policy_direct(j):
        src, place = policy_at(j, f), copies.place()
        copies.start(src, src, to_x, place=place)
        copies.start(src, src, to_y, place=place)
        p_direct[j] = copies.arrival(pg.at[pl.ds(0, 2 * block)], to_x, place)

    def policy_onward(j):
        p_direct[j].wait_recv()
        place = copies.place()
        copies.start(policy_at(j, fx, 0, hb), policy_at(j, fx, 0, hb), to_y, place=place)
        copies.start(policy_at(j, fy, hb, hb), policy_at(j, fy, hb, hb), to_x, place=place)
        p_onward[j] = copies.arrival(pg.at[pl.ds(0, block)], to_x, place)

    def rows_of(slot):
        ahead = jnp.where(
            slot == 0, 3, jnp.where(slot == 1, 2, jnp.where((slot == 2) == end, 1, 0))
        )
        return jnp.where(r >= 2, 3 - ahead, ahead)

    def product(c, slot):
        rows = pl.ds(pl.multiple_of(rows_of(slot) * mine, mine), mine)
        return jnp.dot(x[rows, :], wg[:, col[c]], preferred_element_type=jnp.float32)

    def hop(c, slot, place, device):
        return pltpu.make_async_remote_copy(
            src_ref=snd.at[slot, :, col[c]], dst_ref=inb.at[place, :, col[c]],
            send_sem=z_send.at[slot, c % HOPS], recv_sem=z_recv.at[z_place(place), c],
            device_id=device, device_id_type=MESH,
        )

    def z_place(place):
        return (0, 1, 3, 2, 3)[place]

    def came(c, place):
        hop(c, 0, place, to_near).wait_recv()

    def came_last(c):
        both = inb.at[pl.ds(0, 2), :, col[c]]
        pair = pltpu.make_async_remote_copy(
            src_ref=both, dst_ref=both, send_sem=z_send.at[0, 0], recv_sem=z_recv.at[3, c],
            device_id=to_near, device_id_type=MESH,
        )
        pl.when(mid)(pair.wait_recv)
        pl.when(end)(hop(c, 0, 2, to_near).wait_recv)

    def work_end(*several):
        def one(slot, _):
            for c in several:
                snd[slot, :, col[c]] = product(c, slot).astype(jnp.bfloat16)
                pltpu.make_async_remote_copy(
                    src_ref=snd.at[slot, :, col[c]], dst_ref=inb.at[slot, :, col[c]],
                    send_sem=z_send.at[slot, c % HOPS], recv_sem=z_recv.at[jnp.where(slot == 2, 3, slot), c],
                    device_id=to_near, device_id_type=MESH,
                ).start()
            return 0

        lax.fori_loop(0, 3, one, 0)
        for c in several:
            fin[:, col[c]] = product(c, 3)

    def work_mid(c):
        here = pl.ds(0, wide[c])

        def one(slot, _):
            own[slot_of(c), slot, :, here] = product(c, slot)
            return 0

        lax.fori_loop(0, 3, one, 0)
        fin[:, col[c]] = product(c, 3)

    def work_one(c):
        if c >= 1:
            work_back(c - 1)
        work_across(c)

    def work_two(c):
        work_across(c)
        if c >= 1:
            work_back(c - 1)

    def work_across(*several):
        for slot in range(2):
            for c in several:
                relay(c, slot, slot, 3 + slot, to_across)

    def last_one():
        relay(n - 2, 0, 0, 3, to_across)
        relay(n - 1, 0, 0, 3, to_across)
        work_back(n - 2)
        work_back(n - 1)
        finish(n - 4)
        relay(n - 2, 1, 1, 4, to_across)
        relay(n - 1, 1, 1, 4, to_across)

    def last_two():
        work_across(n - 2, n - 1)
        work_back(n - 3)

    def last_back():
        work_back(n - 2)
        work_back(n - 1)

    def relay(c, slot, source, place, device):
        came(c, source)
        total = own[slot_of(c), slot, :, pl.ds(0, wide[c])] + inb[source, :, col[c]].astype(jnp.float32)
        snd[slot, :, col[c]] = total.astype(jnp.bfloat16)
        hop(c, slot, place, device).start()

    def work_back(c):
        relay(c, 2, 3, 2, to_near)

    def slot_of(c):
        return c % 3

    def summed(at):
        return (
            fin[:, at] + inb[2, :, at].astype(jnp.float32)
            + inb[4, :, at].astype(jnp.float32) + bias[at][None, :]
        )

    def rotated(values):
        return values * cosine[...] + pltpu.roll(values, HD // 2, 1) * sine[...]

    kv_up, kv_on = {}, {}

    def stored(kind, g):
        return pl.ds((2 * g + (kind == "v")) * HD, HD)

    def span(c):
        _, heads = chunks[c]
        return pl.ds((2 * heads[0][1] + (heads[0][0] == "v")) * HD, wide[c])

    key_chunks = [c for c in range(n) if chunks[c][1][0][0] != "q"]
    low, middle, high = (pl.ds(k * mine, mine) for k in range(3))

    def finish_keys(c):
        at, heads = chunks[c]
        for kind, g, j in heads:
            values = summed(pl.ds(at + (j - heads[0][2]) * HD, HD))
            kv[high, stored(kind, g)] = (rotated(values) if kind == "k" else values).astype(jnp.bfloat16)
        kv_up[c] = copies.start(kv.at[high, span(c)], kv.at[middle, span(c)], to_up, r <= 2)

    def forward_keys(c):
        only(r >= 1, kv_up[c].wait_recv)
        kv_on[c] = copies.start(kv.at[middle, span(c)], kv.at[low, span(c)], to_up, mid)

    scale = 1.0 / math.sqrt(HD)
    keys_in = set()

    def attend(c):
        at, heads = chunks[c]
        _, g, first = heads[0]
        for k in key_chunks:
            if k not in keys_in and chunks[k][1][0][1] == g:
                keys_in.add(k)
                only(r >= 2, kv_on[k].wait_recv)
        kc, vc = stored("k", g), stored("v", g)
        base = (g * share + first) * HD

        def head(j, _):
            query = rotated(summed(pl.ds(pl.multiple_of(at + j * HD, HD), HD))).astype(jnp.bfloat16)
            scores = lax.dot_general(
                query, kv[:, kc], (((1,), (1,)), ((), ())), preferred_element_type=jnp.float32
            ) * scale + shut[...]
            expo = jnp.exp(scores - jnp.max(scores, axis=-1, keepdims=True))
            total = jnp.sum(expo, axis=-1, keepdims=True)
            weights = (expo * (1.0 / total)).astype(jnp.bfloat16)
            to = pl.ds(pl.multiple_of(base + j * HD, HD), HD)
            ctx[:, to] = jnp.dot(weights, kv[:, vc], preferred_element_type=jnp.float32).astype(jnp.bfloat16)
            return 0

        lax.fori_loop(0, len(heads), head, 0)
        part = pl.ds(base, wide[c])
        pltpu.make_async_copy(ctx.at[:, part], out.at[:, part], local.at[3]).start()

    def finish(c):
        came_last(c)
        (attend if chunks[c][1][0][0] == "q" else finish_keys)(c)

    def prepare():
        at = pl.ds(pl.multiple_of(r * mine, mine), mine)
        square = (mine, mine)
        row, lane = lax.broadcasted_iota(jnp.int32, square, 0), lax.broadcasted_iota(jnp.int32, square, 1)
        mine_row = jnp.broadcast_to(seg[:, at].astype(jnp.float32), square)
        my_seg = jnp.sum(jnp.where(row == lane, mine_row, 0.0), axis=-1, keepdims=True)
        before = jnp.where(seg[...].astype(jnp.float32) < my_seg, 1.0, 0.0)
        first = jnp.sum(before, axis=-1, keepdims=True)
        index = lax.broadcasted_iota(jnp.int32, (mine, HD), 0) + r * mine
        half = HD // 2
        place = lax.rem(lax.broadcasted_iota(jnp.int32, (1, HD), 1), half)
        freq = jnp.ones((1, HD), jnp.float32)
        for i in range(1, half):
            freq = jnp.where(place == i, 1000000.0 ** (-2.0 * i / HD), freq)
        angle = (index.astype(jnp.float32) - first) * freq
        cosine[...] = jnp.cos(angle)
        wave = jnp.sin(angle)
        sine[...] = jnp.where(lax.broadcasted_iota(jnp.int32, (mine, HD), 1) < half, -wave, wave)
        for slot in range(3):
            there = r - 2 + slot
            keys = pl.ds(pl.multiple_of(jnp.maximum(there, 0) * mine, mine), mine)
            allowed = (my_seg == seg[:, keys].astype(jnp.float32)) & (there >= 0)
            if slot == 2:
                allowed = allowed & (lane <= row)
            shut[:, slot * mine:(slot + 1) * mine] = jnp.where(allowed, 0.0, -1e30)

        @pl.when(r <= 1)
        def _():
            kv[low, :] = jnp.zeros((mine, kv.shape[1]), kv.dtype)

        @pl.when(r == 0)
        def _():
            kv[middle, :] = jnp.zeros((mine, kv.shape[1]), kv.dtype)

        @pl.when(end)
        def _():
            inb[4] = jnp.zeros(inb.shape[1:], inb.dtype)

    def weights_in(c):
        onwards[c].wait_recv()

    queries = len(key_chunks)
    direct(0)
    load_p.wait()
    policy_z(1)
    keep_p = pltpu.make_async_copy(pv, policy_at(r, f), local.at[2])
    keep_p.start()
    left(last_direct[0])
    direct(1)
    onward(0)
    onward(1)
    load_x.wait()
    weights_in(0)
    direct(2)
    pl.when(end)(functools.partial(work_end, 0))
    policy_steps = {
        queries - 1: [("d", 0)], queries: [("d", 1)], queries + 1: [("o", 0), ("d", 2)], queries + 2: [("o", 1)],
        queries + 3: [("d", 3), ("o", 2)], queries + 5: [("o", 3)],
    }

    weight_steps = {0: "o2 d3", 1: "o3 d4", 2: "o4 d5", 3: "o5 d6 d7", 4: "o6 o7 d8 d9"}

    def weights_on(c):
        for word in weight_steps.get(c, f"o{c + 3} d{c + 5}").split():
            if int(word[1:]) < n:
                (direct if word[0] == "d" else onward)(int(word[1:]))

    def sends_out(c):
        for slot in range(3):
            hop(c, slot, 0, to_near).wait_send()

    for c in range(n - 2):
        ahead = [c + 1] if c < n - 3 else [n - 2, n - 1]
        for k in ahead:
            if k >= HOPS:
                sends_out(k - HOPS)
        if 0 <= c - 4 < queries:
            forward_keys(c - 4)
        early = c - 2 < queries - 2
        if 0 <= c - 2 < queries and not early:
            finish(c - 2)
        for k in ahead:
            weights_in(k)
        pl.when(end)(functools.partial(work_end, *ahead))
        if 0 <= c - 2 and early:
            finish(c - 2)
        if c < 3:
            weights_on(c)
        if c == 0:
            prepare()
            policy_z(2)
        if c == 2:
            policy_z(3)
        pl.when(mid)(functools.partial(work_mid, c))
        pl.when(r == 1)(functools.partial(work_one, c))
        pl.when(r == 2)(functools.partial(work_two, c))
        if c == n - 3:
            for k in ahead:
                pl.when(mid)(functools.partial(work_mid, k))
            pl.when(r == 1)(functools.partial(work_back, c))
        if c >= 3:
            weights_on(c)
        if c == queries - 1:
            landed_z(3)
            keep_p.wait()
        for kind, j in policy_steps.get(c, ()):
            (policy_direct if kind == "d" else policy_onward)(j)
        if queries <= c - 2:
            finish(c - 2)
    for j in range(4):
        p_onward[j].wait_recv()
    copies.retire(len(copies.made))
    for c in range(n - HOPS, n - 3):
        sends_out(c)
    pl.when(r == 1)(last_one)
    pl.when(r == 2)(last_two)
    pl.when(r != 1)(functools.partial(finish, n - 4))
    finish(n - 3)
    pl.when(r == 2)(last_back)
    finish(n - 2)
    finish(n - 1)
    for c in range(n - 3, n):
        sends_out(c)
    pltpu.make_async_copy(ctx, out, local.at[3]).wait()


def settle_kernel(ctx, pg, out, whole, store):
    step = pg.shape[0] // PIECES
    stores = [(pg.at[pl.ds(k * step, step)], whole.at[pl.ds(k * step, step)]) for k in range(PIECES)] + [(ctx, out)]
    stores = [pltpu.make_async_copy(src, dst, store.at[i]) for i, (src, dst) in enumerate(stores)]
    for copy in stores:
        copy.start()
    for copy in stores:
        copy.wait()


def whole_layer(tokens, ref_qkv, ref_bias, segment_ids, policy_key):
    rows, depth = tokens.shape
    block, columns = ref_qkv.shape
    mine, share = rows // 4, QH // KVH
    groups = columns // ((share + 2) * HD)
    chunks = plan(groups, share)
    n = len(chunks)
    keys = sum(heads[0][0] != "q" for _, heads in chunks)
    widest = max(len(heads) for _, heads in chunks) * HD
    places = 2 * n + 6 + 2 * keys + 8
    hbm, vmem = pl.BlockSpec(memory_space=pltpu.HBM), pl.BlockSpec(memory_space=pltpu.VMEM)
    any_space = pl.BlockSpec(memory_space=pl.ANY)
    low, full = jnp.bfloat16, jnp.float32
    dma = pltpu.SemaphoreType.DMA
    out, pg = pl.pallas_call(
        layer_kernel,
        out_shape=(
            pltpu.VMEM((mine, groups * share * HD), low),
            pltpu.VMEM((16 * block, policy_key.shape[1]), policy_key.dtype),
        ),
        in_specs=[hbm, hbm, vmem, vmem, hbm],
        out_specs=(any_space, any_space),
        scratch_shapes=[
            pltpu.VMEM((rows, depth), tokens.dtype),
            pltpu.VMEM((4 * block, columns), ref_qkv.dtype),
            pltpu.VMEM((3, 3, mine, widest), full),
            pltpu.VMEM((mine, columns), full),
            pltpu.VMEM((3, mine, columns), low),
            pltpu.VMEM((5, mine, columns), low),
            pltpu.VMEM((3 * mine, groups * 2 * HD), low),
            pltpu.VMEM((mine, 3 * mine), full),
            pltpu.VMEM((mine, HD), full),
            pltpu.VMEM((mine, HD), full),
            pltpu.VMEM((mine, groups * share * HD), low),
            pltpu.VMEM(policy_key.shape, policy_key.dtype),
            dma((RING,)),
            dma((places,)),
            dma((4,)),
            dma((4,)),
            dma((3, HOPS)),
            dma((4, n)),
        ],
        compiler_params=pltpu.CompilerParams(
            collective_id=0, has_side_effects=True, vmem_limit_bytes=VMEM_LIMIT
        ),
    )(tokens, ref_qkv, ref_bias, segment_ids, policy_key)
    return pl.pallas_call(
        settle_kernel,
        out_shape=tuple(jax.ShapeDtypeStruct(a.shape, a.dtype) for a in (out, pg)),
        in_specs=[any_space] * 2,
        out_specs=(any_space,) * 2,
        scratch_shapes=[dma((PIECES + 1,))],
        compiler_params=pltpu.CompilerParams(vmem_limit_bytes=VMEM_LIMIT),
    )(*(pltpu.with_memory_space_constraint(a, pltpu.VMEM) for a in (out, pg)))


PIECES = 4
VMEM_LIMIT = 50 * 1024 * 1024
RING = 32
HOPS = 4


def solution(mesh):
    in_specs = (
        P("fsdp", "rep"),
        P(("rep", "fsdp"), "tp"),
        P("tp"),
        P("fsdp", None),
        P(("rep", "fsdp"), "tp"),
    )
    out_specs = (P(("fsdp", "rep"), "tp"), P(None, "tp"))
    shape = mesh.shape
    grouped = shape["rep"] == 4 and shape["fsdp"] == 4 and shape["tp"] == 2
    return jax.shard_map(
        whole_layer if grouped else per_device, mesh=mesh, in_specs=in_specs, out_specs=out_specs, check_vma=False
    )
```
